128 devices in a mesh: node: 32 (over x, z, core), local: 4 (over y).
Axes of the slice: x: 4, y: 4, z: 4, core: 2. Of those that a mesh axis runs over, the one named last changes fastest.
Arguments:
- tokens: bfloat16 [8192, 5120], P(('node', 'local')), may hold values from -6 to 6
- node_ids: int32 [8192, 3], P(('node', 'local')), may hold values from 0 to 31, as said below
- expert_ids: int32 [8192, 6], P(('node', 'local')), may hold values from 0 to 95, as said below
- gate_weights: bfloat16 [8192, 6], P(('node', 'local')), may hold values from 0.049804688 to 1
- up_weight: bfloat16 [96, 5120, 1536], P('node', None, 'local'), may hold values from -0.078125 to 0.078125
- down_weight: bfloat16 [96, 1536, 5120], P('node', 'local'), may hold values from -0.15625 to 0.15625
Outputs:
- routed_out: bfloat16 [8192, 5120], P(('node', 'local'))
The draws below stay inside these ranges and needn't reach their ends.
Inputs may be any that keep to these rules, and one draw needn't show every extreme that they name: `node_ids`: each token names 3 different nodes; the 64 tokens of one device name every node exactly 6 times. Node m holds experts 3 * m to 3 * m + 2. For each j, expert_ids[t, 2 * j] and expert_ids[t, 2 * j + 1] are two different experts of node node_ids[t, j].
All inputs are finite; a program needn't handle non-finite values.
Results may differ from the reference program's by a relative error of at most 0.012.
Values may be sent and summed in bfloat16 or wider, within the bound.
A program may use at most 192 MiB of HBM per device.

```python
import math
import jax
import jax.numpy as jnp
from jax import lax

D = 5120
FF = 1536
EXP_NODE = 3
TOPK = 6
NODES_SEL = 3
TOK_DEV = 64
TOKENS = 8192
EXPERTS = 96
CAP = 6
N_NODE = 32
N_LOCAL = 4


def routing_tables(key):
    blocks_total = TOKENS // TOK_DEV
    node_total = EXPERTS // EXP_NODE
    base_key = jax.random.fold_in(key, 11)

    def one_block(block_key):
        key_order, key_tokens, key_skip = jax.random.split(block_key, 3)
        node_order = jax.random.permutation(key_order, node_total).astype(jnp.int32)
        cycled = node_order[jnp.arange(NODES_SEL * TOK_DEV, dtype=jnp.int32) % node_total]
        triples = cycled.reshape(TOK_DEV, NODES_SEL)
        shuffled = triples[jax.random.permutation(key_tokens, TOK_DEV)]
        skipped = jax.random.randint(key_skip, (TOK_DEV, NODES_SEL), 0, EXP_NODE).astype(jnp.int32)
        return (shuffled, skipped)
    node_table, skip_table = jax.vmap(one_block)(jax.random.split(base_key, blocks_total))
    return (node_table.reshape(TOKENS, NODES_SEL), skip_table.reshape(TOKENS, NODES_SEL))


def draw_node_ids(key, part):
    node_table, skip_table = routing_tables(key)
    return node_table.astype(jnp.int32)


def draw_expert_ids(key, part):
    node_table, skip_table = routing_tables(key)
    first_pick = (skip_table + 1) % EXP_NODE
    second = (skip_table + 2) % EXP_NODE
    paired = jnp.stack([node_table * EXP_NODE + first_pick, node_table * EXP_NODE + second], axis=2)
    return paired.reshape(TOKENS, TOPK).astype(jnp.int32)


def shard_levels(stream_key, extent, cuts, low, largest):
    loudness = 1.0
    for axis_at, parts in cuts:
        heights = jax.random.uniform(jax.random.fold_in(jax.random.fold_in(stream_key, 6), axis_at), (parts,), jnp.float32, low / len(cuts), largest / len(cuts))
        loudness = loudness * jnp.repeat(jnp.exp(heights), extent[axis_at] // parts).reshape((-1,) + (1,) * (len(extent) - 1 - axis_at))
    return loudness


def bell_draw(key, dims, width, bound, pieces=(), kind=jnp.bfloat16):
    factor_of = shard_levels(key, dims, pieces, -0.22, 0.18) if pieces else 1.0
    values = jax.random.normal(key, dims, jnp.float32) * width * factor_of
    return jnp.minimum(jnp.maximum(values, -bound), bound).astype(kind)


def setup_inputs(seed: int = 0) -> dict:
    key_list = jax.random.split(jax.random.key(seed), 7)
    return {
        "tokens": bell_draw(key_list[0], (TOKENS, D), 1.0, 6.0, ((0, 128),)),
        "node_ids": draw_node_ids(jax.random.fold_in(key_list[6], 71), 0),
        "expert_ids": draw_expert_ids(jax.random.fold_in(key_list[6], 71), 0),
        "gate_weights": jnp.clip(jnp.exp(math.log(1.0) - 2.9996462 * jax.random.uniform(key_list[3], (TOKENS, TOPK), jnp.float32) ** shard_levels(key_list[3], (TOKENS, TOPK), ((0, 128),), -0.2, 0.2)), 0.049804688, 1.0).astype(jnp.bfloat16),
        "up_weight": bell_draw(key_list[4], (EXPERTS, D, FF), D ** -0.5, 0.078125, ((0, 32), (2, 4))),
        "down_weight": bell_draw(key_list[5], (EXPERTS, FF, D), FF ** -0.5, 0.15625, ((0, 32), (1, 4))),
    }


def reference(tokens, node_ids, expert_ids, gate_weights, up_weight, down_weight):
    row_total = N_NODE * N_LOCAL * CAP
    shard_size = FF // N_LOCAL

    def per_node(running, node_id):
        chosen = jnp.any(node_ids == node_id, axis=1)
        row_index = jnp.nonzero(chosen, size=row_total, fill_value=0)[0].astype(jnp.int32)
        picked = tokens[row_index]
        row_experts = expert_ids[row_index]
        row_gates = gate_weights[row_index].astype(jnp.float32)
        contrib = jnp.zeros((row_total, D), jnp.float32)
        for shard_index in range(N_LOCAL):
            partial_value = jnp.zeros((row_total, D), jnp.float32)
            for expert_slot in range(EXP_NODE):
                expert = node_id * EXP_NODE + expert_slot
                weight = jnp.sum(jnp.where(row_experts == expert, row_gates, jnp.float32(0.0)), axis=1)
                up_full = lax.dynamic_index_in_dim(up_weight, expert, 0, keepdims=False)
                down_full = lax.dynamic_index_in_dim(down_weight, expert, 0, keepdims=False)
                up_slice = up_full[:, shard_index * shard_size:(shard_index + 1) * shard_size]
                down_slice = down_full[shard_index * shard_size:(shard_index + 1) * shard_size, :]
                lifted = jnp.dot(picked, up_slice, preferred_element_type=jnp.float32)
                scaled = (jax.nn.silu(lifted) * weight[:, None]).astype(jnp.bfloat16)
                partial_value = partial_value + jnp.dot(scaled, down_slice, preferred_element_type=jnp.float32)
            contrib = contrib + partial_value.astype(jnp.bfloat16).astype(jnp.float32)
        running = running.at[row_index].add(contrib.astype(jnp.bfloat16).astype(jnp.float32))
        return running, None

    final_sum, unused = lax.scan(per_node, jnp.zeros((TOKENS, D), jnp.float32), jnp.arange(N_NODE, dtype=jnp.int32))
    return final_sum.astype(jnp.bfloat16)
```

```python
import functools

import jax
import jax.numpy as jnp
from jax import lax
from jax.experimental import pallas as pl
from jax.experimental.pallas import tpu as pltpu
from jax.sharding import PartitionSpec as P

SLICE = 768
F32 = jnp.float32
BF16 = jnp.bfloat16


def kernel(cfg, tok, nid, eid, gw, up, down, out, *scr):
    n_node, n_loc, cap, n_exp, tr, d_model, ff, a, b = cfg
    (tA, ya, yb, ym, sel, selT, sendA, sendB, xa, xb, upv, dnv, hs, pa, pb, r1d, r1u, r2d, r2u, acc, retA, retB, fA, fB, oA, oB,
     tok_sem, w_sem, y_s, y_r, a_s, a_r, b_s, b_r, ag_s, ag_r, rs_s, rs_r, ra_s, ra_r, rb_s, rb_r, f_s, f_r) = scr
    rows = tr * 8
    cpn = n_loc * cap // 8
    blk = cpn * 8
    slots = n_node * blk
    ng = 4
    gn = n_node // ng
    gc = gn * cpn
    gr = gn * blk
    half = a // 2
    toks = n_loc * rows

    me = lax.axis_index("node")
    y = lax.axis_index("local")
    mx = me // gn
    yu = lax.rem(y + 1, n_loc)
    yd = lax.rem(y + n_loc - 1, n_loc)
    yo = lax.rem(y + 2, n_loc)

    def ncopy(src, dst, ss, rs, m):
        return pltpu.make_async_remote_copy(src, dst, ss, rs, device_id={"node": m}, device_id_type=pl.DeviceIdType.MESH)

    def ycopy(src, dst, ss, rs, p):
        return pltpu.make_async_remote_copy(src, dst, ss, rs, device_id={"local": p}, device_id_type=pl.DeviceIdType.MESH)

    barrier = pltpu.get_barrier_semaphore()

    @pl.loop(1, n_node)
    def _(d):
        pl.semaphore_signal(barrier, 1, device_id={"node": lax.rem(me + d, n_node)}, device_id_type=pl.DeviceIdType.MESH)

    @pl.loop(1, n_loc)
    def _(d):
        pl.semaphore_signal(barrier, 1, device_id={"local": lax.rem(y + d, n_loc)}, device_id_type=pl.DeviceIdType.MESH)

    def tok_copies():
        cs = [pltpu.make_async_copy(tok.at[:, :, pl.ds(s * a, a)], tA.at[s], tok_sem.at[s]) for s in range(n_loc)]
        cs.append(pltpu.make_async_copy(tok.at[:, :, pl.ds(pl.multiple_of(y * a, 128), a)], ya.at[y], tok_sem.at[n_loc]))
        cs.append(pltpu.make_async_copy(tok.at[:, :, pl.ds(n_loc * a, b)], yb.at[y], tok_sem.at[n_loc + 1]))
        return cs

    tcs = tok_copies()
    for c in tcs:
        c.start()
    ws = []
    for e in range(n_exp):
        ws.append(pltpu.make_async_copy(up.at[e], upv.at[:, pl.ds(e * ff, ff)], w_sem.at[e]))
        ws.append(pltpu.make_async_copy(down.at[e], dnv.at[pl.ds(e * ff, ff), :], w_sem.at[n_exp + e]))

    lane = lax.broadcasted_iota(jnp.int32, (rows, 128), 1)
    picked = jnp.zeros((rows, 128), F32)
    for k in range(nid.shape[1]):
        picked = jnp.where(nid[:, k : k + 1] == lane, 1.0, picked)
    gates = jnp.zeros((rows, 128), F32)
    for k in range(eid.shape[1]):
        gates = gates + jnp.where(eid[:, k : k + 1] == lane - n_node, gw[:, k : k + 1].astype(F32), 0.0)
    before = (lax.broadcasted_iota(jnp.int32, (rows, rows), 1) < lax.broadcasted_iota(jnp.int32, (rows, rows), 0)).astype(F32)
    rank = jnp.dot(before.astype(BF16), picked.astype(BF16), preferred_element_type=F32)
    slot = jnp.where(picked > 0.5, rank + (y * cap).astype(F32), -1.0)
    meta = jnp.where(lane < n_node, slot, gates).astype(BF16)
    ym[y] = meta.reshape(tr, 8, 128)

    pl.semaphore_wait(barrier, n_node - 1 + n_loc - 1)

    def y1(kind, d):
        p = lax.rem(y + d, n_loc)
        src = (ym.at[y], tA.at[p], yb.at[y])[kind]
        dst = (ym.at[y], ya.at[y], yb.at[y])[kind]
        return ycopy(src, dst, y_s.at[kind, d], y_r.at[kind, d], p)

    def y1_in(kind, d):
        p = lax.rem(y + n_loc - d, n_loc)
        dst = (ym.at[p], ya.at[p], yb.at[p])[kind]
        return ycopy(dst, dst, y_s.at[kind, d], y_r.at[kind, d], p)

    for d in (1, 3, 2):
        y1(0, d).start()
    for c in tcs:
        c.wait()
    for d in (2, 1, 3):
        y1(1, d).start()
    for d in (2, 1, 3):
        y1(2, d).start()
    for c in ws:
        c.start()

    def gray(k):
        return k + (k // 2) * (1 - 2 * lax.rem(k, 2))

    for d in (1, 3, 2):
        y1_in(0, d).wait_recv()
    mall = ym[...].reshape(toks, 128)
    ex = (lax.broadcasted_iota(jnp.int32, (n_node, blk, 128), 0) == lax.broadcasted_iota(jnp.int32, (n_node, blk, 128), 2)).astype(F32)
    ex = ex.reshape(slots, 128).astype(BF16)
    pick = lax.dot_general(ex, mall, (((1,), (1,)), ((), ())), preferred_element_type=F32)
    want = lax.broadcasted_iota(jnp.int32, (n_node, blk, toks), 1).astype(F32).reshape(slots, toks)
    sel[...] = jnp.where(pick == want, 1.0, 0.0).astype(BF16)
    pickT = lax.dot_general(mall, ex, (((1,), (1,)), ((), ())), preferred_element_type=F32)
    ln = lax.broadcasted_iota(jnp.int32, (toks, slots), 1).astype(F32)
    wantT = ln - blk * jnp.floor((ln + 0.5) * (1.0 / blk))
    selT[...] = jnp.where(pickT == wantT, 1.0, 0.0).astype(BF16)

    def a_out(m):
        return ncopy(sendA.at[pl.ds(m * cpn, cpn)], xa.at[y, pl.ds(me * cpn, cpn)], a_s.at[m], a_r.at[me], m)

    def a_in(m):
        dst = xa.at[y, pl.ds(m * cpn, cpn)]
        return ncopy(dst, dst, a_s.at[m], a_r.at[m], m)

    def b_out(m):
        return ncopy(sendB.at[pl.ds(m * cpn, cpn)], xb.at[pl.ds(me * cpn, cpn)], b_s.at[m], b_r.at[me], m)

    def b_in(m):
        dst = xb.at[pl.ds(m * cpn, cpn)]
        return ncopy(dst, dst, b_s.at[m], b_r.at[m], m)

    def each(g, fn):
        @pl.loop(0, gn)
        def _(j):
            m = g * gn + lax.rem(me + j, gn)

            @pl.when(m != me)
            def _():
                fn(m)

    for d in (1, 3, 2):
        y1_in(1, d).wait_recv()

    @pl.loop(0, ng)
    def _(k):
        g = lax.rem(mx + gray(k), ng)
        rs_ = pl.ds(pl.multiple_of(g * gr, 16), gr)
        val = jnp.dot(sel[rs_, :], ya[...].reshape(toks, a), preferred_element_type=F32)
        sendA[pl.ds(g * gc, gc)] = val.astype(BF16).reshape(gc, 8, a)
        each(g, lambda m: a_out(m).start())

    xa[y, pl.ds(me * cpn, cpn)] = sendA[pl.ds(me * cpn, cpn)]

    for d in (1, 3, 2):
        y1_in(2, d).wait_recv()

    @pl.loop(0, ng)
    def _(k):
        g = lax.rem(mx + gray(k), ng)
        rs_ = pl.ds(pl.multiple_of(g * gr, 16), gr)
        val = jnp.dot(sel[rs_, :], ym[...].reshape(toks, 128), preferred_element_type=F32)
        sendB[pl.ds(g * gc, gc), :, pl.ds(b, 128)] = val.astype(BF16).reshape(gc, 8, 128)
        val = jnp.dot(sel[rs_, :], yb[...].reshape(toks, b), preferred_element_type=F32)
        sendB[pl.ds(g * gc, gc), :, pl.ds(0, b)] = val.astype(BF16).reshape(gc, 8, b)
        each(g, lambda m: b_out(m).start())

    xb[pl.ds(me * cpn, cpn)] = sendB[pl.ds(me * cpn, cpn)]

    lo = pl.ds(0, half)
    hi = pl.ds(half, half)

    def ag(kind, k, g):
        gs = pl.ds(g * gc, gc)
        if kind == 0:
            src, p = xa.at[y, gs], yu
        elif kind == 1:
            src, p = xa.at[y, gs], yd
        elif kind == 2:
            src, p = xa.at[yd, gs, :, lo], yu
        else:
            src, p = xa.at[yu, gs, :, hi], yd
        return ycopy(src, src, ag_s.at[kind, k], ag_r.at[kind, k], p)

    def ag_in(kind, k, g):
        gs = pl.ds(g * gc, gc)
        dst = (xa.at[yd, gs], xa.at[yu, gs], xa.at[yo, gs, :, lo], xa.at[yo, gs, :, hi])[kind]
        return ycopy(dst, dst, ag_s.at[kind, k], ag_r.at[kind, k], y)

    def rs(kind, k, g):
        gs = pl.ds(g * gc, gc)
        if kind == 0:
            src, dst, p = pa.at[yo, gs, :, lo], r1d.at[gs], yu
        elif kind == 1:
            src, dst, p = pa.at[yo, gs, :, hi], r1u.at[gs], yd
        elif kind == 2:
            src, dst, p = pa.at[yu, gs], r2d.at[gs], yu
        else:
            src, dst, p = pa.at[yd, gs], r2u.at[gs], yd
        return ycopy(src, dst, rs_s.at[kind, k], rs_r.at[kind, k], p)

    def rs_in(kind, k, g):
        gs = pl.ds(g * gc, gc)
        dst = (r1d, r1u, r2d, r2u)[kind].at[gs]
        return ycopy(dst, dst, rs_s.at[kind, k], rs_r.at[kind, k], y)

    def ra_out(m):
        return ncopy(acc.at[pl.ds(m * cpn, cpn)], retA.at[pl.ds(me * cpn, cpn)], ra_s.at[m], ra_r.at[me], m)

    def ra_in(m):
        dst = retA.at[pl.ds(m * cpn, cpn)]
        return ncopy(dst, dst, ra_s.at[m], ra_r.at[m], m)

    def rb_out(m):
        return ncopy(pb.at[pl.ds(m * cpn, cpn)], retB.at[pl.ds(me * cpn, cpn)], rb_s.at[m], rb_r.at[me], m)

    def rb_in(m):
        dst = retB.at[pl.ds(m * cpn, cpn)]
        return ncopy(dst, dst, rb_s.at[m], rb_r.at[m], m)

    for c in ws:
        c.wait()

    btile = 512

    def experts(g):
        gs = pl.ds(g * gc, gc)
        glane = lax.broadcasted_iota(jnp.int32, (gr, 128), 1)
        gall = xb[gs, :, pl.ds(b, 128)].astype(F32).reshape(gr, 128)

        @pl.loop(0, n_exp)
        def _(e):
            cs = pl.ds(pl.multiple_of(e * ff, 128), ff)
            v = jnp.zeros((gr, ff), F32)
            for s in range(n_loc):
                v = v + jnp.dot(xa[s, gs].reshape(gr, a), upv[pl.ds(s * a, a), cs], preferred_element_type=F32)
            v = v + jnp.dot(xb[gs, :, pl.ds(0, b)].reshape(gr, b), upv[pl.ds(n_loc * a, b), cs], preferred_element_type=F32)
            gate = jnp.sum(jnp.where(glane == n_node + me * n_exp + e, gall, 0.0), axis=1, keepdims=True)
            hs[:, cs] = (v / (1.0 + jnp.exp(-v)) * gate).astype(BF16)

        @pl.loop(0, n_loc)
        def _(s):
            v = jnp.dot(hs[...], dnv[:, pl.ds(pl.multiple_of(s * a, 128), a)], preferred_element_type=F32)
            pa[s, gs] = v.astype(BF16).reshape(gc, 8, a)

        @pl.loop(0, b // btile)
        def _(t):
            v = jnp.dot(hs[...], dnv[:, pl.ds(pl.multiple_of(n_loc * a + t * btile, 128), btile)], preferred_element_type=F32)
            pb[gs, :, pl.ds(pl.multiple_of(t * btile, 128), btile)] = v.astype(BF16).reshape(gc, 8, btile)

    def group_in(k):
        return lax.rem(mx + ng - gray(k), ng)

    @pl.loop(0, ng + 5)
    def _(i):
        @pl.when(i < ng)
        def _():
            k = i
            g = group_in(k)
            each(g, lambda m: a_in(m).wait_recv())
            ag(0, k, g).start()
            ag(1, k, g).start()

        @pl.when(jnp.logical_and(i >= 1, i < ng + 1))
        def _():
            k = i - 1
            g = group_in(k)
            ag_in(0, k, g).wait_recv()
            ag(2, k, g).start()
            ag_in(1, k, g).wait_recv()
            ag(3, k, g).start()

        @pl.when(jnp.logical_and(i >= 2, i < ng + 2))
        def _():
            k = i - 2
            g = group_in(k)
            each(g, lambda m: b_in(m).wait_recv())
            ag_in(2, k, g).wait_recv()
            ag_in(3, k, g).wait_recv()
            experts(g)
            rs(0, k, g).start()
            rs(1, k, g).start()
            each(g, lambda m: rb_out(m).start())

        @pl.when(jnp.logical_and(i >= 3, i < ng + 3))
        def _():
            k = i - 3
            g = group_in(k)
            gs = pl.ds(g * gc, gc)
            rs_in(0, k, g).wait_recv()
            pa[yu, gs, :, lo] = (pa[yu, gs, :, lo].astype(F32) + r1d[gs].astype(F32)).astype(BF16)
            rs(2, k, g).start()
            rs_in(1, k, g).wait_recv()
            pa[yd, gs, :, hi] = (pa[yd, gs, :, hi].astype(F32) + r1u[gs].astype(F32)).astype(BF16)
            rs(3, k, g).start()

        @pl.when(jnp.logical_and(i >= 4, i < ng + 4))
        def _():
            k = i - 4
            g = group_in(k)
            gs = pl.ds(g * gc, gc)
            rs_in(2, k, g).wait_recv()
            rs_in(3, k, g).wait_recv()
            acc[gs] = (pa[y, gs].astype(F32) + r2d[gs].astype(F32) + r2u[gs].astype(F32)).astype(BF16)
            each(g, lambda m: ra_out(m).start())

    mine = pl.ds(me * cpn, cpn)
    retB[mine] = pb[mine]
    retA[mine] = acc[mine]

    def fin(kind, d):
        p = lax.rem(y + d, n_loc)
        return ycopy((fA, fB)[kind].at[p], (oA, oB)[kind].at[y], f_s.at[kind, d], f_r.at[kind, d], p)

    def fin_in(kind, d):
        p = lax.rem(y + n_loc - d, n_loc)
        dst = (oA, oB)[kind].at[p]
        return ycopy(dst, dst, f_s.at[kind, d], f_r.at[kind, d], p)

    for k in range(ng):
        each(lax.rem(mx + gray(k), ng), lambda m: rb_in(m).wait_recv())

    @pl.loop(0, b // btile)
    def _(t):
        cs = pl.ds(pl.multiple_of(t * btile, 128), btile)
        v = jnp.dot(selT[...], retB[:, :, cs].reshape(slots, btile), preferred_element_type=F32)
        fB[:, :, :, cs] = v.astype(BF16).reshape(n_loc, tr, 8, btile)

    for d in (2, 1, 3):
        fin(1, d).start()
    for k in range(ng):
        each(lax.rem(mx + gray(k), ng), lambda m: ra_in(m).wait_recv())
    v = jnp.dot(selT[...], retA[...].reshape(slots, a), preferred_element_type=F32)
    fA[...] = v.astype(BF16).reshape(n_loc, tr, 8, a)
    for d in (2, 1, 3):
        fin(0, d).start()
    oA[y] = fA[y]
    oB[y] = fB[y]
    for d in (1, 3, 2):
        fin_in(1, d).wait_recv()
    tot = oB[0].astype(F32)
    for s in range(1, n_loc):
        tot = tot + oB[s].astype(F32)
    out[:, :, pl.ds(n_loc * a, b)] = tot.astype(BF16)
    for d in (1, 3, 2):
        fin_in(0, d).wait_recv()
    for s in range(n_loc):
        out[:, :, pl.ds(s * a, a)] = oA[s]

    for d in range(1, n_loc):
        for kind in range(3):
            y1(kind, d).wait_send()
        for kind in range(2):
            fin(kind, d).wait_send()

    @pl.loop(0, ng)
    def _(k):
        g = group_in(k)
        each(g, lambda m: (a_out(m).wait_send(), b_out(m).wait_send(), ra_out(m).wait_send(), rb_out(m).wait_send()) and None)
        for kind in range(4):
            ag(kind, k, g).wait_send()
            rs(kind, k, g).wait_send()


def body(tokens, node_ids, expert_ids, gate_weights, up_weight, down_weight):
    rows, d_model = tokens.shape
    n_node, n_loc = lax.axis_size("node"), lax.axis_size("local")
    n_exp, _, ff = up_weight.shape
    cap = node_ids.shape[1] * rows // n_node
    tr = rows // 8
    a = SLICE
    b = d_model - n_loc * a
    nb = n_node * n_loc * cap // 8
    cfg = (n_node, n_loc, cap, n_exp, tr, d_model, ff, a, b)
    slots = nb * 8
    toks = n_loc * rows
    v = lambda *s: pltpu.VMEM(s, BF16)
    dma = lambda *s: pltpu.SemaphoreType.DMA(s)
    scratch = [
        v(n_loc, tr, 8, a),
        v(n_loc, tr, 8, a),
        v(n_loc, tr, 8, b),
        v(n_loc, tr, 8, 128),
        v(slots, toks),
        v(toks, slots),
        v(nb, 8, a),
        v(nb, 8, b + 128),
        v(n_loc, nb, 8, a),
        v(nb, 8, b + 128),
        v(d_model, n_exp * ff),
        v(n_exp * ff, d_model),
        v(slots // 4, n_exp * ff),
        v(n_loc, nb, 8, a),
        v(nb, 8, b),
        v(nb, 8, a // 2),
        v(nb, 8, a // 2),
        v(nb, 8, a),
        v(nb, 8, a),
        v(nb, 8, a),
        v(nb, 8, a),
        v(nb, 8, b),
        v(n_loc, tr, 8, a),
        v(n_loc, tr, 8, b),
        v(n_loc, tr, 8, a),
        v(n_loc, tr, 8, b),
        dma(n_loc + 2),
        dma(2 * n_exp),
        dma(3, n_loc), dma(3, n_loc),
        dma(n_node), dma(n_node),
        dma(n_node), dma(n_node),
        dma(4, 4), dma(4, 4),
        dma(4, 4), dma(4, 4),
        dma(n_node), dma(n_node),
        dma(n_node), dma(n_node),
        dma(2, n_loc), dma(2, n_loc),
    ]
    vm = pl.BlockSpec(memory_space=pltpu.VMEM)
    hbm = pl.BlockSpec(memory_space=pl.ANY)
    out = pl.pallas_call(
        functools.partial(kernel, cfg),
        out_shape=jax.ShapeDtypeStruct((tr, 8, d_model), BF16),
        in_specs=[hbm, vm, vm, vm, hbm, hbm],
        out_specs=vm,
        scratch_shapes=scratch,
        compiler_params=pltpu.CompilerParams(collective_id=0, has_side_effects=True, vmem_limit_bytes=67043328),
    )(tokens.reshape(tr, 8, d_model), node_ids, expert_ids, gate_weights, up_weight, down_weight)
    return out.reshape(rows, d_model)


def solution(mesh):
    in_specs = (
        P(("node", "local"), None),
        P(("node", "local"), None),
        P(("node", "local"), None),
        P(("node", "local"), None),
        P("node", None, "local"),
        P("node", "local", None),
    )
    out_specs = P(("node", "local"), None)
    return jax.shard_map(body, mesh=mesh, in_specs=in_specs, out_specs=out_specs, check_vma=False)
```

```python
import functools

import jax
import jax.numpy as jnp
from jax import lax
from jax.experimental import pallas as pl
from jax.experimental.pallas import tpu as pltpu
from jax.sharding import PartitionSpec as P

SLICE = 768
F32 = jnp.float32
BF16 = jnp.bfloat16


def kernel(cfg, tok, nid, eid, gw, up, down, out, *scr):
    n_node, n_loc, cap, n_exp, tr, ff, a, b = cfg
    (tA, yb, ym, selA, selAT, sel, selT, turn, xs, ps, sA, sB, xa, xb, upv, dnv, hs, r1d, r1u, r2d, r2u, retA, retB, fB, oB,
     tok_sem, w_sem, y_s, y_r, x_s, x_r, z_s, z_r, ag_s, ag_r, rs_s, rs_r, rz_s, rz_r, rx_s, rx_r, f_s, f_r) = scr
    rows = tr * 8
    cpn = n_loc * cap // 8
    blk = cpn * 8
    slots = n_node * blk
    ng = 4
    nz = 4
    gn = n_node // ng
    gc = gn * cpn
    gr = gn * blk
    lo_w = (a // 128 + 1) // 2 * 128
    lo = pl.ds(0, lo_w)
    hi = pl.ds(lo_w, a - lo_w)
    toks = n_loc * rows
    hid = n_exp * ff
    btile = 512
    near = (0, 1, 3, 2)

    me = lax.axis_index("node")
    y = lax.axis_index("local")
    mx = me // gn
    q = lax.rem(me, gn)
    mz = q // 2
    mc = lax.rem(q, 2)
    yu = lax.rem(y + 1, n_loc)
    yd = lax.rem(y + n_loc - 1, n_loc)
    yo = lax.rem(y + 2, n_loc)

    def gray(k):
        return k + (k // 2) * (1 - 2 * (k % 2)) if isinstance(k, int) else k + (k // 2) * (1 - 2 * lax.rem(k, 2))

    def group_out(k):
        return lax.rem(mx + gray(k), ng)

    def group_in(k):
        return lax.rem(mx + ng - gray(k), ng)

    def stage(k):
        far = (k + 3) // 4
        return mx * (1 - far) + (ng + k - 1) * far

    def peer_out(p, h):
        return 2 * lax.rem(mz + near[p], nz) + lax.rem(mc + h, 2)

    def cells(n):
        return pl.ds(n * cpn, cpn)

    def ncopy(src, dst, ss, rs, m):
        return pltpu.make_async_remote_copy(src, dst, ss, rs, device_id={"node": m}, device_id_type=pl.DeviceIdType.MESH)

    def ycopy(src, dst, ss, rs, p):
        return pltpu.make_async_remote_copy(src, dst, ss, rs, device_id={"local": p}, device_id_type=pl.DeviceIdType.MESH)

    barrier = pltpu.get_barrier_semaphore()
    for d in (2, 1, 3):
        pl.semaphore_signal(barrier, 1, device_id={"local": lax.rem(y + d, n_loc)}, device_id_type=pl.DeviceIdType.MESH)
    for d in (2, 1, 3):
        pl.semaphore_signal(barrier, 1, device_id={"node": lax.rem(mx + d, ng) * gn + q}, device_id_type=pl.DeviceIdType.MESH)
    for d in (4, 5, 3, 2, 6, 7, 1):
        pl.semaphore_signal(barrier, 1, device_id={"node": mx * gn + lax.rem(q + d, gn)}, device_id_type=pl.DeviceIdType.MESH)

    tcs = [pltpu.make_async_copy(tok.at[:, :, pl.ds(s * a, a)], tA.at[s], tok_sem.at[s]) for s in range(n_loc)]
    tcs.append(pltpu.make_async_copy(tok.at[:, :, pl.ds(n_loc * a, b)], yb.at[y], tok_sem.at[n_loc]))
    for c in tcs:
        c.start()
    ws = []
    for e in range(n_exp):
        ws.append(pltpu.make_async_copy(up.at[e], upv.at[:, pl.ds(e * ff, ff)], w_sem.at[e]))
        ws.append(pltpu.make_async_copy(down.at[e], dnv.at[pl.ds(e * ff, ff), :], w_sem.at[n_exp + e]))

    sub = lax.broadcasted_iota(jnp.int32, (128, rows), 0)
    picked = jnp.zeros((128, rows), F32)
    for k in range(nid.shape[0]):
        picked = jnp.where(nid[k : k + 1, :] == sub, 1.0, picked)
    gates = jnp.zeros((128, rows), F32)
    gwf = gw[...].astype(F32)
    for k in range(eid.shape[0]):
        gates = gates + jnp.where(eid[k : k + 1, :] == sub - n_node, gwf[k : k + 1, :], 0.0)
    i0 = lax.broadcasted_iota(jnp.int32, (rows, rows), 0)
    i1 = lax.broadcasted_iota(jnp.int32, (rows, rows), 1)
    before = jnp.where(i0 < i1, 1.0, 0.0).astype(BF16)
    rank = jnp.dot(picked.astype(BF16), before, preferred_element_type=F32)
    metaT = jnp.where(sub < n_node, jnp.where(picked > 0.5, rank, -1.0), gates).astype(BF16)
    eye = jnp.where(i0 == i1, 1.0, 0.0).astype(BF16)
    meta = lax.dot_general(eye, metaT, (((1,), (1,)), ((), ())), preferred_element_type=F32)
    slot_lane = lax.broadcasted_iota(jnp.int32, (rows, 128), 1) < n_node

    def shifted(n):
        return jnp.where(jnp.logical_and(slot_lane, meta > -0.5), meta + n * cap, meta).astype(BF16)

    def placing(mall, ref, refT):
        ex = (lax.broadcasted_iota(jnp.int32, (n_node, blk, 128), 0) == lax.broadcasted_iota(jnp.int32, (n_node, blk, 128), 2)).astype(F32)
        ex = ex.reshape(slots, 128).astype(BF16)
        pick = lax.dot_general(ex, mall, (((1,), (1,)), ((), ())), preferred_element_type=F32)
        want = lax.broadcasted_iota(jnp.int32, (n_node, blk, toks), 1).astype(F32).reshape(slots, toks)
        ref[...] = jnp.where(pick == want, 1.0, 0.0).astype(BF16)
        pickT = lax.dot_general(mall, ex, (((1,), (1,)), ((), ())), preferred_element_type=F32)
        ln = lax.broadcasted_iota(jnp.int32, (toks, slots), 1).astype(F32)
        wantT = ln - blk * jnp.floor((ln + 0.5) * (1.0 / blk))
        refT[...] = jnp.where(pickT == wantT, 1.0, 0.0).astype(BF16)

    ym[y] = shifted(y.astype(F32)).reshape(tr, 8, 128)
    placing(jnp.concatenate([shifted(float(s)) for s in range(n_loc)], axis=0), selA, selAT)
    for c in tcs:
        c.wait()
    for k in range(ng):
        gs = group_out(k)
        v = jnp.dot(selA[pl.ds(pl.multiple_of(gs * gr, 16), gr), :], tA[...].reshape(toks, a), preferred_element_type=F32)
        sA[pl.ds(gs * gc, gc)] = v.astype(BF16).reshape(gc, 8, a)

    with jax.named_scope("barrier"):
        pl.semaphore_wait(barrier, n_loc - 1 + ng - 1 + gn - 1)

    ybuf = (ym, yb)

    def spread_tokens(kind):
        for d in (2, 1, 3):
            p = lax.rem(y + d, n_loc)
            ycopy(ybuf[kind].at[y], ybuf[kind].at[y], y_s.at[kind], y_r.at[kind], p).start()

    def all_tokens(kind):
        ref = ybuf[kind].at[pl.ds(0, n_loc - 1)]
        return ycopy(ref, ref, y_s.at[kind], y_r.at[kind], y)

    spread_tokens(0)
    spread_tokens(1)

    sbuf = (sA, sB)

    def land(kind, n):
        return xa.at[y, cells(n)] if kind == 0 else xb.at[cells(n)]

    def xleg(kind, k, p):
        z = lax.rem(mz + near[p], nz)
        src = sbuf[kind].at[pl.ds((group_out(k) * gn + 2 * z) * cpn, 2 * cpn)]
        dst = sbuf[kind].at[pl.ds((stage(k) * gn + 2 * z) * cpn, 2 * cpn)]
        return ncopy(src, dst, x_s.at[kind, k - 1, p], x_r.at[kind, k - 1, p], group_out(k) * gn + q)

    def zleg(kind, k, p, h):
        to = peer_out(p, h)
        src = sbuf[kind].at[cells(stage(k) * gn + to)]
        return ncopy(src, land(kind, group_in(k) * gn + q), z_s.at[kind, k], z_r.at[kind, k], mx * gn + to)

    def all_forwarded(kind, k):
        dst = xa.at[y, pl.ds(0, (gn - 1) * cpn)] if kind == 0 else xb.at[pl.ds(0, (gn - 1) * cpn)]
        return ncopy(sbuf[kind].at[pl.ds(0, (gn - 1) * cpn)], dst, z_s.at[kind, k], z_r.at[kind, k], me)

    def forward(kind, k, p):
        if k > 0:
            xleg(kind, k, p).wait_recv()
        if p > 0:
            zleg(kind, k, p, 0).start()
        zleg(kind, k, p, 1).start()
        if p == 0:
            n = group_in(k) * gn + q
            if kind == 0:
                xa[y, cells(n)] = sA[cells(stage(k) * gn + q)]
            else:
                xb[cells(n)] = sB[cells(stage(k) * gn + q)]

    def arrived(kind, k):
        all_forwarded(kind, k).wait_recv()

    def near_leg(kind, k):
        for p in range(nz):
            xleg(kind, k, p).start()

    def select(k):
        g = group_out(k)
        pick_rows = sel[pl.ds(pl.multiple_of(g * gr, 16), gr), :]
        gs = pl.ds(g * gc, gc)
        v = jnp.dot(pick_rows, ym[...].reshape(toks, 128), preferred_element_type=F32)
        sB[gs, :, pl.ds(b, 128)] = v.astype(BF16).reshape(gc, 8, 128)
        v = jnp.dot(pick_rows, yb[...].reshape(toks, b), preferred_element_type=F32)
        sB[gs, :, pl.ds(0, b)] = v.astype(BF16).reshape(gc, 8, b)

    def far_leg(kind, *ps):
        for p in ps:
            xleg(kind, 3, p).start()

    def ag(kind, k):
        gs = pl.ds(group_in(k) * gc, gc)
        if kind == 0:
            src, p = xa.at[y, gs], yu
        elif kind == 1:
            src, p = xa.at[y, gs], yd
        elif kind == 2:
            src, p = xa.at[yd, gs, :, lo], yu
        else:
            src, p = xa.at[yu, gs, :, hi], yd
        return ycopy(src, src, ag_s.at[kind, k], ag_r.at[kind, k], p)

    def ag_in(kind, k):
        gs = pl.ds(group_in(k) * gc, gc)
        dst = (xa.at[yd, gs], xa.at[yu, gs], xa.at[yo, gs, :, lo], xa.at[yo, gs, :, hi])[kind]
        return ycopy(dst, dst, ag_s.at[kind, k], ag_r.at[kind, k], y)

    def spread(k):
        with jax.named_scope("spread"):
            arrived(0, k)
            ag(0, k).start()
            ag(1, k).start()

    def spread_far(k):
        with jax.named_scope("spread_far"):
            ag_in(0, k).wait_recv()
            ag(2, k).start()
            ag_in(1, k).wait_recv()
            ag(3, k).start()

    def rs(kind, k):
        gs = pl.ds(group_in(k) * gc, gc)
        if kind == 0:
            src, dst, p = xa.at[yo, gs, :, lo], r1d.at[gs], yu
        elif kind == 1:
            src, dst, p = xa.at[yo, gs, :, hi], r1u.at[gs], yd
        elif kind == 2:
            src, dst, p = xa.at[yu, gs], r2d.at[gs], yu
        else:
            src, dst, p = xa.at[yd, gs], r2u.at[gs], yd
        return ycopy(src, dst, rs_s.at[kind, k], rs_r.at[kind, k], p)

    def rs_in(kind, k):
        dst = (r1d, r1u, r2d, r2u)[kind].at[pl.ds(group_in(k) * gc, gc)]
        return ycopy(dst, dst, rs_s.at[kind, k], rs_r.at[kind, k], y)

    rbuf = (retA, retB)

    def result(kind, n, count):
        n = pl.ds(n * cpn, count * cpn)
        return xa.at[y, n] if kind == 0 else xb.at[n, :, pl.ds(0, b)]

    def rx(kind, k, p):
        z = lax.rem(mz + near[p], nz)
        src = result(kind, group_in(k) * gn + 2 * z, 2)
        dst = rbuf[kind].at[pl.ds((stage(k) * gn + 2 * z) * cpn, 2 * cpn)]
        return ncopy(src, dst, rx_s.at[kind, k - 1, p], rx_r.at[kind, k - 1, p], group_in(k) * gn + q)

    def rz(kind, k, p, h):
        to = peer_out(p, h)
        src = result(kind, mx * gn + to, 1) if k == 0 else rbuf[kind].at[cells(stage(k) * gn + to)]
        dst = rbuf[kind].at[cells(group_out(k) * gn + q)]
        return ncopy(src, dst, rz_s.at[kind, k], rz_r.at[kind, k], mx * gn + to)

    def all_back(kind, k):
        ref = rbuf[kind].at[pl.ds(0, (gn - 1) * cpn)]
        return ncopy(ref, ref, rz_s.at[kind, k], rz_r.at[kind, k], me)

    def back(kind, k, p):
        with jax.named_scope("back%d" % kind):
            if k > 0:
                rx(kind, k, p).wait_recv()
            if p > 0:
                rz(kind, k, p, 0).start()
            rz(kind, k, p, 1).start()
            if p == 0:
                to = cells(group_out(k) * gn + q)
                if k > 0:
                    rbuf[kind][to] = rbuf[kind][cells(stage(k) * gn + q)]
                elif kind == 0:
                    retA[to] = xa[y, to]
                else:
                    retB[to] = xb[to, :, pl.ds(0, b)]

    def sum_far(k):
        gs = pl.ds(group_in(k) * gc, gc)
        with jax.named_scope("sum_far"):
            rs_in(0, k).wait_recv()
            xa[yu, gs, :, lo] = (xa[yu, gs, :, lo].astype(F32) + r1d[gs].astype(F32)).astype(BF16)
            rs(2, k).start()
            rs_in(1, k).wait_recv()
            xa[yd, gs, :, hi] = (xa[yd, gs, :, hi].astype(F32) + r1u[gs].astype(F32)).astype(BF16)
            rs(3, k).start()

    def sum_near(k):
        gs = pl.ds(group_in(k) * gc, gc)
        with jax.named_scope("sum_near"):
            rs_in(2, k).wait_recv()
            rs_in(3, k).wait_recv()
            xa[y, gs] = (xa[y, gs].astype(F32) + r2d[gs].astype(F32) + r2u[gs].astype(F32)).astype(BF16)
        for p in (1, 2, 3, 0):
            if k == 0:
                back(0, 0, p)
            else:
                rx(0, k, p).start()

    def experts(k):
        g = group_in(k)
        gs = pl.ds(g * gc, gc)
        glane = lax.broadcasted_iota(jnp.int32, (gr, 128), 1)
        gall = xb[gs, :, pl.ds(b, 128)].astype(F32).reshape(gr, 128)
        gate = [jnp.sum(jnp.where(glane == n_node + me * n_exp + e, gall, 0.0), axis=1, keepdims=True) for e in range(n_exp)]
        planes = jnp.concatenate([xa[s, gs].reshape(gr, a) for s in range(n_loc)], axis=0)
        for s in range(n_loc):
            xs[:, pl.ds(s * a, a)] = jnp.dot(turn[s], planes, preferred_element_type=F32).astype(BF16)
        x = jnp.concatenate([xs[...], xb[gs, :, pl.ds(0, b)].reshape(gr, b)], axis=1)
        for c in range(0, hid, 256):
            w = min(256, hid - c)
            v = jnp.dot(x, upv[:, pl.ds(c, w)], preferred_element_type=F32)
            for j in range(0, w, 128):
                u = v[:, j : j + 128]
                hs[:, pl.ds(c + j, 128)] = (u / (1.0 + jnp.exp(-u)) * gate[(c + j) // ff]).astype(BF16)
        for s in range(n_loc):
            v = jnp.dot(hs[...], dnv[:, pl.ds(s * a, a)], preferred_element_type=F32)
            ps[pl.ds(s * gr, gr), :] = v.astype(BF16)
        for c in range(0, b, btile):
            v = jnp.dot(hs[...], dnv[:, pl.ds(n_loc * a + c, btile)], preferred_element_type=F32)
            xb[gs, :, pl.ds(c, btile)] = v.astype(BF16).reshape(gc, 8, btile)
        for s in range(n_loc):
            v = jnp.dot(turn[s], ps[...], preferred_element_type=F32)
            xa[s, gs] = v.astype(BF16).reshape(gc, 8, a)

    def relay(kind, *ks):
        def steps(p):
            with jax.named_scope("relay%d" % kind):
                for k in ks:
                    forward(kind, k, p)
        return steps

    for k in (1, 2):
        near_leg(0, k)
    for p in range(nz):
        forward(0, 0, p)
    for c in ws:
        c.start()
    place = lax.broadcasted_iota(jnp.int32, (gn, blk, n_loc * gr), 1).astype(F32)
    node_row = lax.broadcasted_iota(jnp.int32, (gn, blk, n_loc * gr), 0).astype(F32)
    column = lax.broadcasted_iota(jnp.int32, (gn, blk, n_loc * gr), 2).astype(F32)
    first = jnp.floor((place + 0.5) * (1.0 / cap)) * (gr - cap) + place + node_row * blk
    for s in range(n_loc):
        turn[s] = jnp.where(column == first + s * cap, 1.0, 0.0).reshape(gr, n_loc * gr).astype(BF16)
    with jax.named_scope("wait_meta"):
        all_tokens(0).wait_recv()
    placing(ym[...].reshape(toks, 128), sel, selT)
    for p in range(nz):
        relay(0, 1, 2)(p)
    far_leg(0, 0, 1, 2, 3)
    spread(0)
    with jax.named_scope("wait_yB"):
        all_tokens(1).wait_recv()
    for k in (1, 2):
        select(k)
        near_leg(1, k)
    select(0)
    for p in range(nz):
        forward(1, 0, p)
    select(3)
    for p in range(nz):
        relay(0, 3)(p)
    spread(1)
    spread_far(0)
    relay(1, 1, 2)(0)
    spread(2)
    relay(1, 1, 2)(1)
    spread_far(1)
    relay(1, 1, 2)(2)
    spread(3)
    relay(1, 1, 2)(3)
    far_leg(1, 0, 1, 2, 3)
    for c in ws:
        c.wait()

    def ready(k):
        with jax.named_scope("ready_b"):
            arrived(1, k)
        with jax.named_scope("ready_a"):
            ag_in(2, k).wait_recv()
            ag_in(3, k).wait_recv()
            for kind in range(4):
                ag(kind, k).wait_send()

    def after(k):
        rs(0, k).start()
        rs(1, k).start()
        for p in (1, 2, 3, 0):
            if k == 0:
                back(1, 0, p)
            else:
                rx(1, k, p).start()

    @pl.loop(0, ng)
    def _(i):
        for k in range(ng):
            @pl.when(i == k)
            def _():
                ready(k)

        with jax.named_scope("experts"):
            experts(i)

        @pl.when(i == 0)
        def _():
            spread_far(2)
            after(0)
            relay(1, 3)(0)
            relay(1, 3)(1)

        @pl.when(i == 1)
        def _():
            after(1)
            spread_far(3)
            relay(1, 3)(2)
            relay(1, 3)(3)
            sum_far(0)

        @pl.when(i == 2)
        def _():
            after(2)
            sum_far(1)

        @pl.when(i == 3)
        def _():
            after(3)

    sum_near(0)
    sum_far(2)
    back(1, 1, 0)
    back(1, 1, 1)
    back(1, 1, 2)
    sum_near(1)
    back(1, 2, 0)
    back(1, 1, 3)
    back(1, 2, 1)
    sum_far(3)
    back(1, 2, 2)
    back(1, 2, 3)
    sum_near(2)
    back(1, 3, 0)
    back(1, 3, 1)
    sum_near(3)
    back(1, 3, 2)
    back(1, 3, 3)
    for p in range(nz):
        back(0, 1, p)

    def fin_all():
        return ycopy(fB.at[pl.ds(0, n_loc - 1)], oB.at[pl.ds(0, n_loc - 1)], f_s.at[0], f_r.at[0], y)

    def returned(kind):
        with jax.named_scope("returned%d" % kind):
            for k in range(ng):
                all_back(kind, k).wait_recv()

    returned(1)
    for c in range(0, b, btile):
        cs = pl.ds(c, btile)
        v = jnp.dot(selT[...], retB[pl.ds(0, slots // 8), :, cs].reshape(slots, btile), preferred_element_type=F32)
        fB[:, :, :, cs] = v.astype(BF16).reshape(n_loc, tr, 8, btile)
    for d in (2, 1, 3):
        p = lax.rem(y + d, n_loc)
        ycopy(fB.at[p], oB.at[y], f_s.at[0], f_r.at[0], p).start()
    oB[y] = fB[y]
    for k in (2, 3):
        for p in range(nz):
            back(0, k, p)
    with jax.named_scope("wait_finB"):
        fin_all().wait_recv()
    tot = oB[0].astype(F32)
    for s in range(1, n_loc):
        tot = tot + oB[s].astype(F32)
    out[:, :, pl.ds(n_loc * a, b)] = tot.astype(BF16)
    returned(0)
    v = jnp.dot(selAT[...], retA[pl.ds(0, slots // 8)].reshape(slots, a), preferred_element_type=F32)
    v = v.astype(BF16).reshape(n_loc, tr, 8, a)
    for s in range(n_loc):
        out[:, :, pl.ds(s * a, a)] = v[s]

    with jax.named_scope("drain"):
        fin_all().wait_send()
        for kind in range(2):
            all_tokens(kind).wait_send()
            for k in range(ng):
                all_forwarded(kind, k).wait_send()
                all_back(kind, k).wait_send()
                for p in range(nz):
                    if k > 0:
                        xleg(kind, k, p).wait_send()
                        rx(kind, k, p).wait_send()
        for k in range(ng):
            for kind in range(4):
                rs(kind, k).wait_send()


def body(tokens, node_ids, expert_ids, gate_weights, up_weight, down_weight):
    rows, d_model = tokens.shape
    n_node, n_loc = lax.axis_size("node"), lax.axis_size("local")
    n_exp, _, ff = up_weight.shape
    cap = node_ids.shape[1] * rows // n_node
    tr = rows // 8
    a = SLICE
    b = d_model - n_loc * a
    nb = n_node * n_loc * cap // 8
    cfg = (n_node, n_loc, cap, n_exp, tr, ff, a, b)
    slots = nb * 8
    toks = n_loc * rows
    v = lambda *s: pltpu.VMEM(s, BF16)
    dma = lambda *s: pltpu.SemaphoreType.DMA(s)
    two_legs = nb // 4 * 7
    lo_w = (a // 128 + 1) // 2 * 128
    scratch = [
        v(n_loc, tr, 8, a),
        v(n_loc, tr, 8, b),
        v(n_loc, tr, 8, 128),
        v(slots, toks),
        v(toks, slots),
        v(slots, toks),
        v(toks, slots),
        v(n_loc, slots // 4, slots),
        v(slots // 4, n_loc * a),
        v(slots, a),
        v(two_legs, 8, a),
        v(two_legs, 8, b + 128),
        v(n_loc, nb, 8, a),
        v(nb, 8, b + 128),
        v(d_model, n_exp * ff),
        v(n_exp * ff, d_model),
        v(slots // 4, n_exp * ff),
        v(nb, 8, lo_w),
        v(nb, 8, a - lo_w),
        v(nb, 8, a),
        v(nb, 8, a),
        v(two_legs, 8, a),
        v(two_legs, 8, b),
        v(n_loc, tr, 8, b),
        v(n_loc, tr, 8, b),
        dma(n_loc + 1),
        dma(2 * n_exp),
        dma(2), dma(2),
        dma(2, 3, 4), dma(2, 3, 4),
        dma(2, 4), dma(2, 4),
        dma(4, 4), dma(4, 4),
        dma(4, 4), dma(4, 4),
        dma(2, 4), dma(2, 4),
        dma(2, 3, 4), dma(2, 3, 4),
        dma(1), dma(1),
    ]
    vm = pl.BlockSpec(memory_space=pltpu.VMEM)
    hbm = pl.BlockSpec(memory_space=pl.ANY)
    out = pl.pallas_call(
        functools.partial(kernel, cfg),
        out_shape=jax.ShapeDtypeStruct((tr, 8, d_model), BF16),
        in_specs=[hbm, vm, vm, vm, hbm, hbm],
        out_specs=vm,
        scratch_shapes=scratch,
        compiler_params=pltpu.CompilerParams(collective_id=0, has_side_effects=True, vmem_limit_bytes=67043328),
    )(tokens.reshape(tr, 8, d_model), node_ids.T, expert_ids.T, gate_weights.T, up_weight, down_weight)
    return out.reshape(rows, d_model)


def solution(mesh):
    in_specs = (
        P(("node", "local"), None),
        P(("node", "local"), None),
        P(("node", "local"), None),
        P(("node", "local"), None),
        P("node", None, "local"),
        P("node", "local", None),
    )
    out_specs = P(("node", "local"), None)
    return jax.shard_map(body, mesh=mesh, in_specs=in_specs, out_specs=out_specs, check_vma=False)
```

```python
import functools

import jax
import jax.numpy as jnp
from jax import lax
from jax.experimental import pallas as pl
from jax.experimental.pallas import tpu as pltpu
from jax.sharding import PartitionSpec as P

SLICE = 896
F32 = jnp.float32
BF16 = jnp.bfloat16


def kernel(cfg, tok, nid, eid, gw, up, down, out, *scr):
    n_node, n_loc, cap, n_exp, tr, ff, a, b = cfg
    (tA, yb, ym, selA, selAT, sel, selT, turn, xs, ps, sA, sB, xa, xb, upv, dnv, hs, r1d, r1u, r2d, r2u, retA, retB, fB, oB,
     tok_sem, w_sem, y_s, y_r, x_s, x_r, z_s, z_r, ag_s, ag_r, rs_s, rs_r, rz_s, rz_r, rx_s, rx_r, f_s, f_r) = scr
    rows = tr * 8
    cpn = n_loc * cap // 8
    blk = cpn * 8
    slots = n_node * blk
    ng = 4
    nz = 4
    gn = n_node // ng
    gc = gn * cpn
    gr = gn * blk
    lo_w = (a // 128 + 1) // 2 * 128
    lo = pl.ds(0, lo_w)
    hi = pl.ds(lo_w, a - lo_w)
    toks = n_loc * rows
    hid = n_exp * ff
    btile = 512
    near = (0, 1, 3, 2)

    me = lax.axis_index("node")
    y = lax.axis_index("local")
    mx = me // gn
    q = lax.rem(me, gn)
    mz = q // 2
    mc = lax.rem(q, 2)
    yu = lax.rem(y + 1, n_loc)
    yd = lax.rem(y + n_loc - 1, n_loc)
    yo = lax.rem(y + 2, n_loc)

    def gray(k):
        return k + (k // 2) * (1 - 2 * (k % 2)) if isinstance(k, int) else k + (k // 2) * (1 - 2 * lax.rem(k, 2))

    def group_out(k):
        return lax.rem(mx + gray(k), ng)

    def group_in(k):
        return lax.rem(mx + ng - gray(k), ng)

    def stage(k):
        far = (k + 3) // 4
        return mx * (1 - far) + (ng + k - 1) * far

    def peer_out(p, h):
        return 2 * lax.rem(mz + near[p], nz) + lax.rem(mc + h, 2)

    def cells(n):
        return pl.ds(n * cpn, cpn)

    def ncopy(src, dst, ss, rs, m):
        return pltpu.make_async_remote_copy(src, dst, ss, rs, device_id={"node": m}, device_id_type=pl.DeviceIdType.MESH)

    def ycopy(src, dst, ss, rs, p):
        return pltpu.make_async_remote_copy(src, dst, ss, rs, device_id={"local": p}, device_id_type=pl.DeviceIdType.MESH)

    barrier = pltpu.get_barrier_semaphore()
    for d in (2, 1, 3):
        pl.semaphore_signal(barrier, 1, device_id={"local": lax.rem(y + d, n_loc)}, device_id_type=pl.DeviceIdType.MESH)
    for d in (2, 1, 3):
        pl.semaphore_signal(barrier, 1, device_id={"node": lax.rem(mx + d, ng) * gn + q}, device_id_type=pl.DeviceIdType.MESH)
    for d in (4, 5, 3, 2, 6, 7, 1):
        pl.semaphore_signal(barrier, 1, device_id={"node": mx * gn + lax.rem(q + d, gn)}, device_id_type=pl.DeviceIdType.MESH)

    tcs = [pltpu.make_async_copy(tok.at[:, :, pl.ds(s * a, a)], tA.at[s], tok_sem.at[s]) for s in range(n_loc)]
    tcs.append(pltpu.make_async_copy(tok.at[:, :, pl.ds(n_loc * a, b)], yb.at[y], tok_sem.at[n_loc]))
    for c in tcs:
        c.start()
    ws = []
    for e in range(n_exp):
        ws.append(pltpu.make_async_copy(up.at[e], upv.at[:, pl.ds(e * ff, ff)], w_sem.at[e]))
        ws.append(pltpu.make_async_copy(down.at[e], dnv.at[pl.ds(e * ff, ff), :], w_sem.at[n_exp + e]))

    sub = lax.broadcasted_iota(jnp.int32, (128, rows), 0)
    picked = jnp.zeros((128, rows), F32)
    for k in range(nid.shape[0]):
        picked = jnp.where(nid[k : k + 1, :] == sub, 1.0, picked)
    gates = jnp.zeros((128, rows), F32)
    gwf = gw[...].astype(F32)
    for k in range(eid.shape[0]):
        gates = gates + jnp.where(eid[k : k + 1, :] == sub - n_node, gwf[k : k + 1, :], 0.0)
    i0 = lax.broadcasted_iota(jnp.int32, (rows, rows), 0)
    i1 = lax.broadcasted_iota(jnp.int32, (rows, rows), 1)
    before = jnp.where(i0 < i1, 1.0, 0.0).astype(BF16)
    rank = jnp.dot(picked.astype(BF16), before, preferred_element_type=F32)
    metaT = jnp.where(sub < n_node, jnp.where(picked > 0.5, rank, -1.0), gates).astype(BF16)
    eye = jnp.where(i0 == i1, 1.0, 0.0).astype(BF16)
    meta = lax.dot_general(eye, metaT, (((1,), (1,)), ((), ())), preferred_element_type=F32)
    slot_lane = lax.broadcasted_iota(jnp.int32, (rows, 128), 1) < n_node

    def shifted(n):
        return jnp.where(jnp.logical_and(slot_lane, meta > -0.5), meta + n * cap, meta).astype(BF16)

    def placing(mall, ref, refT):
        ex = (lax.broadcasted_iota(jnp.int32, (n_node, blk, 128), 0) == lax.broadcasted_iota(jnp.int32, (n_node, blk, 128), 2)).astype(F32)
        ex = ex.reshape(slots, 128).astype(BF16)
        pick = lax.dot_general(ex, mall, (((1,), (1,)), ((), ())), preferred_element_type=F32)
        want = lax.broadcasted_iota(jnp.int32, (n_node, blk, toks), 1).astype(F32).reshape(slots, toks)
        ref[...] = jnp.where(pick == want, 1.0, 0.0).astype(BF16)
        pickT = lax.dot_general(mall, ex, (((1,), (1,)), ((), ())), preferred_element_type=F32)
        ln = lax.broadcasted_iota(jnp.int32, (toks, slots), 1).astype(F32)
        wantT = ln - blk * jnp.floor((ln + 0.5) * (1.0 / blk))
        refT[...] = jnp.where(pickT == wantT, 1.0, 0.0).astype(BF16)

    ym[y] = shifted(y.astype(F32)).reshape(tr, 8, 128)
    placing(jnp.concatenate([shifted(float(s)) for s in range(n_loc)], axis=0), selA, selAT)
    for c in tcs:
        c.wait()
    for k in range(ng):
        gs = group_out(k)
        v = jnp.dot(selA[pl.ds(pl.multiple_of(gs * gr, 16), gr), :], tA[...].reshape(toks, a), preferred_element_type=F32)
        sA[pl.ds(gs * gc, gc)] = v.astype(BF16).reshape(gc, 8, a)

    with jax.named_scope("barrier"):
        pl.semaphore_wait(barrier, n_loc - 1 + ng - 1 + gn - 1)

    ybuf = (ym, yb)

    def spread_tokens(kind):
        for d in (2, 1, 3):
            p = lax.rem(y + d, n_loc)
            ycopy(ybuf[kind].at[y], ybuf[kind].at[y], y_s.at[kind], y_r.at[kind], p).start()

    def all_tokens(kind):
        ref = ybuf[kind].at[pl.ds(0, n_loc - 1)]
        return ycopy(ref, ref, y_s.at[kind], y_r.at[kind], y)

    spread_tokens(0)
    spread_tokens(1)

    sbuf = (sA, sB)

    def land(kind, n):
        return xa.at[y, cells(n)] if kind == 0 else xb.at[cells(n)]

    def xleg(kind, k, p):
        z = lax.rem(mz + near[p], nz)
        src = sbuf[kind].at[pl.ds((group_out(k) * gn + 2 * z) * cpn, 2 * cpn)]
        dst = sbuf[kind].at[pl.ds((stage(k) * gn + 2 * z) * cpn, 2 * cpn)]
        return ncopy(src, dst, x_s.at[kind, k - 1, p], x_r.at[kind, k - 1, p], group_out(k) * gn + q)

    def zleg(kind, k, p, h):
        to = peer_out(p, h)
        src = sbuf[kind].at[cells(stage(k) * gn + to)]
        return ncopy(src, land(kind, group_in(k) * gn + q), z_s.at[kind, k], z_r.at[kind, k], mx * gn + to)

    def all_forwarded(kind, k):
        dst = xa.at[y, pl.ds(0, (gn - 1) * cpn)] if kind == 0 else xb.at[pl.ds(0, (gn - 1) * cpn)]
        return ncopy(sbuf[kind].at[pl.ds(0, (gn - 1) * cpn)], dst, z_s.at[kind, k], z_r.at[kind, k], me)

    def forward(kind, k, p):
        if k > 0:
            xleg(kind, k, p).wait_recv()
        if p > 0:
            zleg(kind, k, p, 0).start()
        zleg(kind, k, p, 1).start()
        if p == 0:
            n = group_in(k) * gn + q
            if kind == 0:
                xa[y, cells(n)] = sA[cells(stage(k) * gn + q)]
            else:
                xb[cells(n)] = sB[cells(stage(k) * gn + q)]

    def arrived(kind, k):
        all_forwarded(kind, k).wait_recv()

    def near_leg(kind, k):
        for p in range(nz):
            xleg(kind, k, p).start()

    def select(k):
        g = group_out(k)
        pick_rows = sel[pl.ds(pl.multiple_of(g * gr, 16), gr), :]
        gs = pl.ds(g * gc, gc)
        v = jnp.dot(pick_rows, ym[...].reshape(toks, 128), preferred_element_type=F32)
        sB[gs, :, pl.ds(b, 128)] = v.astype(BF16).reshape(gc, 8, 128)
        v = jnp.dot(pick_rows, yb[...].reshape(toks, b), preferred_element_type=F32)
        sB[gs, :, pl.ds(0, b)] = v.astype(BF16).reshape(gc, 8, b)

    def far_leg(kind, *ps):
        for p in ps:
            xleg(kind, 3, p).start()

    def ag(kind, k):
        gs = pl.ds(group_in(k) * gc, gc)
        if kind == 0:
            src, p = xa.at[y, gs], yu
        elif kind == 1:
            src, p = xa.at[y, gs], yd
        elif kind == 2:
            src, p = xa.at[yd, gs, :, lo], yu
        else:
            src, p = xa.at[yu, gs, :, hi], yd
        return ycopy(src, src, ag_s.at[kind, k], ag_r.at[kind, k], p)

    def ag_in(kind, k):
        gs = pl.ds(group_in(k) * gc, gc)
        dst = (xa.at[yd, gs], xa.at[yu, gs], xa.at[yo, gs, :, lo], xa.at[yo, gs, :, hi])[kind]
        return ycopy(dst, dst, ag_s.at[kind, k], ag_r.at[kind, k], y)

    def spread(k):
        with jax.named_scope("spread"):
            arrived(0, k)
            ag(0, k).start()
            ag(1, k).start()

    def spread_far(k):
        with jax.named_scope("spread_far"):
            ag_in(0, k).wait_recv()
            ag(2, k).start()
            ag_in(1, k).wait_recv()
            ag(3, k).start()

    def rs(kind, k):
        gs = pl.ds(group_in(k) * gc, gc)
        if kind == 0:
            src, dst, p = xa.at[yo, gs, :, lo], r1d.at[gs], yu
        elif kind == 1:
            src, dst, p = xa.at[yo, gs, :, hi], r1u.at[gs], yd
        elif kind == 2:
            src, dst, p = xa.at[yu, gs], r2d.at[gs], yu
        else:
            src, dst, p = xa.at[yd, gs], r2u.at[gs], yd
        return ycopy(src, dst, rs_s.at[kind, k], rs_r.at[kind, k], p)

    def rs_in(kind, k):
        dst = (r1d, r1u, r2d, r2u)[kind].at[pl.ds(group_in(k) * gc, gc)]
        return ycopy(dst, dst, rs_s.at[kind, k], rs_r.at[kind, k], y)

    rbuf = (retA, retB)

    def result(kind, n, count):
        n = pl.ds(n * cpn, count * cpn)
        return xa.at[y, n] if kind == 0 else xb.at[n, :, pl.ds(0, b)]

    def rx(kind, k, p):
        z = lax.rem(mz + near[p], nz)
        src = result(kind, group_in(k) * gn + 2 * z, 2)
        dst = rbuf[kind].at[pl.ds((stage(k) * gn + 2 * z) * cpn, 2 * cpn)]
        return ncopy(src, dst, rx_s.at[kind, k - 1, p], rx_r.at[kind, k - 1, p], group_in(k) * gn + q)

    def rz(kind, k, p, h):
        to = peer_out(p, h)
        src = result(kind, mx * gn + to, 1) if k == 0 else rbuf[kind].at[cells(stage(k) * gn + to)]
        dst = rbuf[kind].at[cells(group_out(k) * gn + q)]
        return ncopy(src, dst, rz_s.at[kind, k], rz_r.at[kind, k], mx * gn + to)

    def all_back(kind, k):
        ref = rbuf[kind].at[pl.ds(0, (gn - 1) * cpn)]
        return ncopy(ref, ref, rz_s.at[kind, k], rz_r.at[kind, k], me)

    def back(kind, k, p):
        with jax.named_scope("back%d" % kind):
            if k > 0:
                rx(kind, k, p).wait_recv()
            if p > 0:
                rz(kind, k, p, 0).start()
            rz(kind, k, p, 1).start()
            if p == 0:
                to = cells(group_out(k) * gn + q)
                if k > 0:
                    rbuf[kind][to] = rbuf[kind][cells(stage(k) * gn + q)]
                elif kind == 0:
                    retA[to] = xa[y, to]
                else:
                    retB[to] = xb[to, :, pl.ds(0, b)]

    def sum_far(k):
        gs = pl.ds(group_in(k) * gc, gc)
        with jax.named_scope("sum_far"):
            rs_in(0, k).wait_recv()
            xa[yu, gs, :, lo] = (xa[yu, gs, :, lo].astype(F32) + r1d[gs].astype(F32)).astype(BF16)
            rs(2, k).start()
            rs_in(1, k).wait_recv()
            xa[yd, gs, :, hi] = (xa[yd, gs, :, hi].astype(F32) + r1u[gs].astype(F32)).astype(BF16)
            rs(3, k).start()

    def sum_near(k):
        gs = pl.ds(group_in(k) * gc, gc)
        with jax.named_scope("sum_near"):
            rs_in(2, k).wait_recv()
            rs_in(3, k).wait_recv()
            xa[y, gs] = (xa[y, gs].astype(F32) + r2d[gs].astype(F32) + r2u[gs].astype(F32)).astype(BF16)
        for p in (1, 2, 3, 0):
            if k == 0:
                back(0, 0, p)
            else:
                rx(0, k, p).start()

    def experts(k):
        g = group_in(k)
        gs = pl.ds(g * gc, gc)
        glane = lax.broadcasted_iota(jnp.int32, (gr, 128), 1)
        gall = xb[gs, :, pl.ds(b, 128)].astype(F32).reshape(gr, 128)
        gate = [jnp.sum(jnp.where(glane == n_node + me * n_exp + e, gall, 0.0), axis=1, keepdims=True) for e in range(n_exp)]
        planes = jnp.concatenate([xa[s, gs].reshape(gr, a) for s in range(n_loc)], axis=0)
        for s in range(n_loc):
            xs[:, pl.ds(s * a, a)] = jnp.dot(turn[s], planes, preferred_element_type=F32).astype(BF16)
        x = jnp.concatenate([xs[...], xb[gs, :, pl.ds(0, b)].reshape(gr, b)], axis=1)
        for c in range(0, hid, 256):
            w = min(256, hid - c)
            v = jnp.dot(x, upv[:, pl.ds(c, w)], preferred_element_type=F32)
            for j in range(0, w, 128):
                u = v[:, j : j + 128]
                hs[:, pl.ds(c + j, 128)] = (u / (1.0 + jnp.exp(-u)) * gate[(c + j) // ff]).astype(BF16)
        for s in range(n_loc):
            v = jnp.dot(hs[...], dnv[:, pl.ds(s * a, a)], preferred_element_type=F32)
            ps[pl.ds(s * gr, gr), :] = v.astype(BF16)
        for c in range(0, b, btile):
            v = jnp.dot(hs[...], dnv[:, pl.ds(n_loc * a + c, btile)], preferred_element_type=F32)
            xb[gs, :, pl.ds(c, btile)] = v.astype(BF16).reshape(gc, 8, btile)
        for s in range(n_loc):
            v = jnp.dot(turn[s], ps[...], preferred_element_type=F32)
            xa[s, gs] = v.astype(BF16).reshape(gc, 8, a)

    def relay(kind, *ks):
        def steps(p):
            with jax.named_scope("relay%d" % kind):
                for k in ks:
                    forward(kind, k, p)
        return steps

    for k in (1, 2):
        near_leg(0, k)
    for p in range(nz):
        forward(0, 0, p)
    for c in ws:
        c.start()
    place = lax.broadcasted_iota(jnp.int32, (gn, blk, n_loc * gr), 1).astype(F32)
    node_row = lax.broadcasted_iota(jnp.int32, (gn, blk, n_loc * gr), 0).astype(F32)
    column = lax.broadcasted_iota(jnp.int32, (gn, blk, n_loc * gr), 2).astype(F32)
    first = jnp.floor((place + 0.5) * (1.0 / cap)) * (gr - cap) + place + node_row * blk
    for s in range(n_loc):
        turn[s] = jnp.where(column == first + s * cap, 1.0, 0.0).reshape(gr, n_loc * gr).astype(BF16)
    with jax.named_scope("wait_meta"):
        all_tokens(0).wait_recv()
    placing(ym[...].reshape(toks, 128), sel, selT)
    for p in range(nz):
        relay(0, 1, 2)(p)
    far_leg(0, 0, 1, 2, 3)
    spread(0)
    with jax.named_scope("wait_yB"):
        all_tokens(1).wait_recv()
    for k in (1, 2):
        select(k)
        near_leg(1, k)
    select(0)
    for p in range(nz):
        forward(1, 0, p)
    select(3)
    for p in range(nz):
        relay(0, 3)(p)
    spread(1)
    spread_far(0)
    relay(1, 1, 2)(0)
    spread(2)
    relay(1, 1, 2)(1)
    spread_far(1)
    relay(1, 1, 2)(2)
    spread(3)
    relay(1, 1, 2)(3)
    far_leg(1, 0, 1, 2, 3)
    for c in ws:
        c.wait()

    def ready(k):
        with jax.named_scope("ready_b"):
            arrived(1, k)
        with jax.named_scope("ready_a"):
            ag_in(2, k).wait_recv()
            ag_in(3, k).wait_recv()
            for kind in range(4):
                ag(kind, k).wait_send()

    def after(k):
        if k > 0:
            rs(0, k).start()
            rs(1, k).start()
        for p in (1, 2, 3, 0):
            if k == 0:
                back(1, 0, p)
            else:
                rx(1, k, p).start()

    @pl.loop(0, ng)
    def _(i):
        for k in range(ng):
            @pl.when(i == k)
            def _():
                ready(k)

        with jax.named_scope("experts"):
            experts(i)

        @pl.when(i == 0)
        def _():
            spread_far(2)
            after(0)
            relay(1, 3)(0)

        @pl.when(i == 1)
        def _():
            after(1)
            spread_far(3)
            relay(1, 3)(1)
            relay(1, 3)(2)
            relay(1, 3)(3)

        @pl.when(i == 2)
        def _():
            after(2)
            sum_far(1)
            rs(0, 0).start()
            rs(1, 0).start()
            back(1, 1, 0)
            back(1, 1, 1)
            back(1, 1, 2)

        @pl.when(i == 3)
        def _():
            after(3)

    sum_far(2)
    back(1, 1, 3)
    back(1, 2, 0)
    back(1, 2, 1)
    sum_near(1)
    back(1, 2, 2)
    back(1, 2, 3)
    back(1, 3, 0)
    sum_far(3)
    back(1, 3, 1)
    back(1, 3, 2)
    sum_near(2)
    sum_far(0)
    back(1, 3, 3)
    for p in range(nz):
        back(0, 1, p)
    sum_near(3)

    def fin_all():
        return ycopy(fB.at[pl.ds(0, n_loc - 1)], oB.at[pl.ds(0, n_loc - 1)], f_s.at[0], f_r.at[0], y)

    def returned(kind):
        with jax.named_scope("returned%d" % kind):
            for k in range(ng):
                all_back(kind, k).wait_recv()

    returned(1)
    for c in range(0, b, btile):
        cs = pl.ds(c, btile)
        v = jnp.dot(selT[...], retB[pl.ds(0, slots // 8), :, cs].reshape(slots, btile), preferred_element_type=F32)
        fB[:, :, :, cs] = v.astype(BF16).reshape(n_loc, tr, 8, btile)
    for d in (2, 1, 3):
        p = lax.rem(y + d, n_loc)
        ycopy(fB.at[p], oB.at[y], f_s.at[0], f_r.at[0], p).start()
    oB[y] = fB[y]
    for p in range(nz):
        back(0, 2, p)
    sum_near(0)
    for p in range(nz):
        back(0, 3, p)
    with jax.named_scope("wait_finB"):
        fin_all().wait_recv()
    tot = oB[0].astype(F32)
    for s in range(1, n_loc):
        tot = tot + oB[s].astype(F32)
    out[:, :, pl.ds(n_loc * a, b)] = tot.astype(BF16)
    returned(0)
    v = jnp.dot(selAT[...], retA[pl.ds(0, slots // 8)].reshape(slots, a), preferred_element_type=F32)
    v = v.astype(BF16).reshape(n_loc, tr, 8, a)
    for s in range(n_loc):
        out[:, :, pl.ds(s * a, a)] = v[s]

    with jax.named_scope("drain"):
        fin_all().wait_send()
        for kind in range(2):
            all_tokens(kind).wait_send()
            for k in range(ng):
                all_forwarded(kind, k).wait_send()
                all_back(kind, k).wait_send()
                for p in range(nz):
                    if k > 0:
                        xleg(kind, k, p).wait_send()
                        rx(kind, k, p).wait_send()
        for k in range(ng):
            for kind in range(4):
                rs(kind, k).wait_send()


def body(tokens, node_ids, expert_ids, gate_weights, up_weight, down_weight):
    rows, d_model = tokens.shape
    n_node, n_loc = lax.axis_size("node"), lax.axis_size("local")
    n_exp, _, ff = up_weight.shape
    cap = node_ids.shape[1] * rows // n_node
    tr = rows // 8
    a = SLICE
    b = d_model - n_loc * a
    nb = n_node * n_loc * cap // 8
    cfg = (n_node, n_loc, cap, n_exp, tr, ff, a, b)
    slots = nb * 8
    toks = n_loc * rows
    v = lambda *s: pltpu.VMEM(s, BF16)
    dma = lambda *s: pltpu.SemaphoreType.DMA(s)
    two_legs = nb // 4 * 7
    lo_w = (a // 128 + 1) // 2 * 128
    scratch = [
        v(n_loc, tr, 8, a),
        v(n_loc, tr, 8, b),
        v(n_loc, tr, 8, 128),
        v(slots, toks),
        v(toks, slots),
        v(slots, toks),
        v(toks, slots),
        v(n_loc, slots // 4, slots),
        v(slots // 4, n_loc * a),
        v(slots, a),
        v(two_legs, 8, a),
        v(two_legs, 8, b + 128),
        v(n_loc, nb, 8, a),
        v(nb, 8, b + 128),
        v(d_model, n_exp * ff),
        v(n_exp * ff, d_model),
        v(slots // 4, n_exp * ff),
        v(nb, 8, lo_w),
        v(nb, 8, a - lo_w),
        v(nb, 8, a),
        v(nb, 8, a),
        v(two_legs, 8, a),
        v(two_legs, 8, b),
        v(n_loc, tr, 8, b),
        v(n_loc, tr, 8, b),
        dma(n_loc + 1),
        dma(2 * n_exp),
        dma(2), dma(2),
        dma(2, 3, 4), dma(2, 3, 4),
        dma(2, 4), dma(2, 4),
        dma(4, 4), dma(4, 4),
        dma(4, 4), dma(4, 4),
        dma(2, 4), dma(2, 4),
        dma(2, 3, 4), dma(2, 3, 4),
        dma(1), dma(1),
    ]
    vm = pl.BlockSpec(memory_space=pltpu.VMEM)
    hbm = pl.BlockSpec(memory_space=pl.ANY)
    out = pl.pallas_call(
        functools.partial(kernel, cfg),
        out_shape=jax.ShapeDtypeStruct((tr, 8, d_model), BF16),
        in_specs=[hbm, vm, vm, vm, hbm, hbm],
        out_specs=vm,
        scratch_shapes=scratch,
        compiler_params=pltpu.CompilerParams(collective_id=0, has_side_effects=True, vmem_limit_bytes=67043328),
    )(tokens.reshape(tr, 8, d_model), node_ids.T, expert_ids.T, gate_weights.T, up_weight, down_weight)
    return out.reshape(rows, d_model)


def solution(mesh):
    in_specs = (
        P(("node", "local"), None),
        P(("node", "local"), None),
        P(("node", "local"), None),
        P(("node", "local"), None),
        P("node", None, "local"),
        P("node", "local", None),
    )
    out_specs = P(("node", "local"), None)
    return jax.shard_map(body, mesh=mesh, in_specs=in_specs, out_specs=out_specs, check_vma=False)
```

```python
import functools

import jax
import jax.numpy as jnp
from jax import lax
from jax.experimental import pallas as pl
from jax.experimental.pallas import tpu as pltpu
from jax.sharding import PartitionSpec as P

SLICE = 896
F32 = jnp.float32
BF16 = jnp.bfloat16


def kernel(cfg, tok, nid, eid, gw, up, down, out, *scr):
    n_node, n_loc, cap, n_exp, tr, ff, a, b = cfg
    (tA, yb, ym, selA, selAT, sel, selT, turn, xs, ps, sA, sB, xa, xb, upv, dnv, hs, r1, r2d, r2u, retA, retB, fB, oB,
     tok_sem, w_sem, y_s, y_r, x_s, x_r, z_s, z_r, ag_s, ag_r, rs_s, rs_r, rz_s, rz_r, rx_s, rx_r, f_s, f_r) = scr
    rows = tr * 8
    cpn = n_loc * cap // 8
    blk = cpn * 8
    slots = n_node * blk
    ng = 4
    nz = 4
    gn = n_node // ng
    gc = gn * cpn
    gr = gn * blk
    toks = n_loc * rows
    hid = n_exp * ff
    btile = 512
    near = (0, 1, 3, 2)

    me = lax.axis_index("node")
    y = lax.axis_index("local")
    mx = me // gn
    q = lax.rem(me, gn)
    mz = q // 2
    mc = lax.rem(q, 2)
    yu = lax.rem(y + 1, n_loc)
    yd = lax.rem(y + n_loc - 1, n_loc)
    yo = lax.rem(y + 2, n_loc)

    def gray(k):
        return k + (k // 2) * (1 - 2 * (k % 2)) if isinstance(k, int) else k + (k // 2) * (1 - 2 * lax.rem(k, 2))

    def group_out(k):
        return lax.rem(mx + gray(k), ng)

    def group_in(k):
        return lax.rem(mx + ng - gray(k), ng)

    def stage(k):
        far = (k + 3) // 4
        return mx * (1 - far) + (ng + k - 1) * far

    def peer_out(p, h):
        return 2 * lax.rem(mz + near[p], nz) + lax.rem(mc + h, 2)

    def half(k, h):
        return pl.ds(group_in(k) * gc + h * (gc // 2), gc // 2)

    def cells(n):
        return pl.ds(n * cpn, cpn)

    def ncopy(src, dst, ss, rs, m):
        return pltpu.make_async_remote_copy(src, dst, ss, rs, device_id={"node": m}, device_id_type=pl.DeviceIdType.MESH)

    def ycopy(src, dst, ss, rs, p):
        return pltpu.make_async_remote_copy(src, dst, ss, rs, device_id={"local": p}, device_id_type=pl.DeviceIdType.MESH)

    barrier = pltpu.get_barrier_semaphore()
    for d in (2, 1, 3):
        pl.semaphore_signal(barrier, 1, device_id={"local": lax.rem(y + d, n_loc)}, device_id_type=pl.DeviceIdType.MESH)
    for d in (2, 1, 3):
        pl.semaphore_signal(barrier, 1, device_id={"node": lax.rem(mx + d, ng) * gn + q}, device_id_type=pl.DeviceIdType.MESH)
    for d in (4, 5, 3, 2, 6, 7, 1):
        pl.semaphore_signal(barrier, 1, device_id={"node": mx * gn + lax.rem(q + d, gn)}, device_id_type=pl.DeviceIdType.MESH)

    tcs = [pltpu.make_async_copy(tok.at[:, :, pl.ds(s * a, a)], tA.at[s], tok_sem.at[s]) for s in range(n_loc)]
    tcs.append(pltpu.make_async_copy(tok.at[:, :, pl.ds(n_loc * a, b)], yb.at[y], tok_sem.at[n_loc]))
    for c in tcs:
        c.start()
    ws = []
    for e in range(n_exp):
        ws.append(pltpu.make_async_copy(up.at[e], upv.at[:, pl.ds(e * ff, ff)], w_sem.at[e]))
        ws.append(pltpu.make_async_copy(down.at[e], dnv.at[pl.ds(e * ff, ff), :], w_sem.at[n_exp + e]))

    sub = lax.broadcasted_iota(jnp.int32, (128, rows), 0)
    picked = jnp.zeros((128, rows), F32)
    for k in range(nid.shape[0]):
        picked = jnp.where(nid[k : k + 1, :] == sub, 1.0, picked)
    gates = jnp.zeros((128, rows), F32)
    gwf = gw[...].astype(F32)
    for k in range(eid.shape[0]):
        gates = gates + jnp.where(eid[k : k + 1, :] == sub - n_node, gwf[k : k + 1, :], 0.0)
    i0 = lax.broadcasted_iota(jnp.int32, (rows, rows), 0)
    i1 = lax.broadcasted_iota(jnp.int32, (rows, rows), 1)
    before = jnp.where(i0 < i1, 1.0, 0.0).astype(BF16)
    rank = jnp.dot(picked.astype(BF16), before, preferred_element_type=F32)
    metaT = jnp.where(sub < n_node, jnp.where(picked > 0.5, rank, -1.0), gates).astype(BF16)
    eye = jnp.where(i0 == i1, 1.0, 0.0).astype(BF16)
    meta = lax.dot_general(eye, metaT, (((1,), (1,)), ((), ())), preferred_element_type=F32)
    slot_lane = lax.broadcasted_iota(jnp.int32, (rows, 128), 1) < n_node

    def shifted(n):
        return jnp.where(jnp.logical_and(slot_lane, meta > -0.5), meta + n * cap, meta).astype(BF16)

    def placing(mall, ref, refT):
        ex = (lax.broadcasted_iota(jnp.int32, (n_node, blk, 128), 0) == lax.broadcasted_iota(jnp.int32, (n_node, blk, 128), 2)).astype(F32)
        ex = ex.reshape(slots, 128).astype(BF16)
        pick = lax.dot_general(ex, mall, (((1,), (1,)), ((), ())), preferred_element_type=F32)
        want = lax.broadcasted_iota(jnp.int32, (n_node, blk, toks), 1).astype(F32).reshape(slots, toks)
        ref[...] = jnp.where(pick == want, 1.0, 0.0).astype(BF16)
        pickT = lax.dot_general(mall, ex, (((1,), (1,)), ((), ())), preferred_element_type=F32)
        ln = lax.broadcasted_iota(jnp.int32, (toks, slots), 1).astype(F32)
        wantT = ln - blk * jnp.floor((ln + 0.5) * (1.0 / blk))
        refT[...] = jnp.where(pickT == wantT, 1.0, 0.0).astype(BF16)

    ym[y] = shifted(y.astype(F32)).reshape(tr, 8, 128)
    placing(jnp.concatenate([shifted(float(s)) for s in range(n_loc)], axis=0), selA, selAT)
    for c in tcs:
        c.wait()
    for k in range(ng):
        gs = group_out(k)
        v = jnp.dot(selA[pl.ds(pl.multiple_of(gs * gr, 16), gr), :], tA[...].reshape(toks, a), preferred_element_type=F32)
        sA[pl.ds(gs * gc, gc)] = v.astype(BF16).reshape(gc, 8, a)

    with jax.named_scope("barrier"):
        pl.semaphore_wait(barrier, n_loc - 1 + ng - 1 + gn - 1)

    ybuf = (ym, yb)

    def spread_tokens(kind):
        for d in (2, 1, 3):
            p = lax.rem(y + d, n_loc)
            ycopy(ybuf[kind].at[y], ybuf[kind].at[y], y_s.at[kind], y_r.at[kind], p).start()

    def all_tokens(kind):
        ref = ybuf[kind].at[pl.ds(0, n_loc - 1)]
        return ycopy(ref, ref, y_s.at[kind], y_r.at[kind], y)

    spread_tokens(0)
    spread_tokens(1)

    sbuf = (sA, sB)

    def land(kind, n):
        return xa.at[y, cells(n)] if kind == 0 else xb.at[cells(n)]

    def xleg(kind, k, p):
        z = lax.rem(mz + near[p], nz)
        src = sbuf[kind].at[pl.ds((group_out(k) * gn + 2 * z) * cpn, 2 * cpn)]
        dst = sbuf[kind].at[pl.ds((stage(k) * gn + 2 * z) * cpn, 2 * cpn)]
        return ncopy(src, dst, x_s.at[kind, k - 1, p], x_r.at[kind, k - 1, p], group_out(k) * gn + q)

    def zleg(kind, k, p, h):
        to = peer_out(p, h)
        src = sbuf[kind].at[cells(stage(k) * gn + to)]
        return ncopy(src, land(kind, group_in(k) * gn + q), z_s.at[kind, k], z_r.at[kind, k], mx * gn + to)

    def all_forwarded(kind, k):
        dst = xa.at[y, pl.ds(0, (gn - 1) * cpn)] if kind == 0 else xb.at[pl.ds(0, (gn - 1) * cpn)]
        return ncopy(sbuf[kind].at[pl.ds(0, (gn - 1) * cpn)], dst, z_s.at[kind, k], z_r.at[kind, k], me)

    def forward(kind, k, p):
        if k > 0:
            xleg(kind, k, p).wait_recv()
        if p > 0:
            zleg(kind, k, p, 0).start()
        zleg(kind, k, p, 1).start()
        if p == 0:
            n = group_in(k) * gn + q
            if kind == 0:
                xa[y, cells(n)] = sA[cells(stage(k) * gn + q)]
            else:
                xb[cells(n)] = sB[cells(stage(k) * gn + q)]

    def arrived(kind, k):
        all_forwarded(kind, k).wait_recv()

    def near_leg(kind, k):
        for p in range(nz):
            xleg(kind, k, p).start()

    def select(k):
        g = group_out(k)
        pick_rows = sel[pl.ds(pl.multiple_of(g * gr, 16), gr), :]
        gs = pl.ds(g * gc, gc)
        v = jnp.dot(pick_rows, ym[...].reshape(toks, 128), preferred_element_type=F32)
        sB[gs, :, pl.ds(b, 128)] = v.astype(BF16).reshape(gc, 8, 128)
        v = jnp.dot(pick_rows, yb[...].reshape(toks, b), preferred_element_type=F32)
        sB[gs, :, pl.ds(0, b)] = v.astype(BF16).reshape(gc, 8, b)

    def far_leg(kind, *ps):
        for p in ps:
            xleg(kind, 3, p).start()

    def ag(kind, k):
        gs = pl.ds(group_in(k) * gc, gc)
        if kind == 0:
            src, p = xa.at[y, gs], yu
        elif kind == 1:
            src, p = xa.at[y, gs], yd
        elif kind == 2:
            src, p = xa.at[yd, half(k, 0)], yu
        else:
            src, p = xa.at[yu, half(k, 1)], yd
        return ycopy(src, src, ag_s.at[kind, k], ag_r.at[kind, k], p)

    def ag_in(kind, k):
        gs = pl.ds(group_in(k) * gc, gc)
        dst = (xa.at[yd, gs], xa.at[yu, gs], xa.at[yo, half(k, 0)], xa.at[yo, half(k, 1)])[kind]
        return ycopy(dst, dst, ag_s.at[kind, k], ag_r.at[kind, k], y)

    def spread(k):
        with jax.named_scope("spread"):
            arrived(0, k)
            ag(0, k).start()
            ag(1, k).start()

    def spread_far(k):
        with jax.named_scope("spread_far"):
            ag_in(0, k).wait_recv()
            ag(2, k).start()
            ag_in(1, k).wait_recv()
            ag(3, k).start()

    def rs(kind, k):
        gs = pl.ds(group_in(k) * gc, gc)
        if kind == 0:
            src, dst, p = xa.at[yo, half(k, 0)], r1.at[half(k, 0)], yu
        elif kind == 1:
            src, dst, p = xa.at[yo, half(k, 1)], r1.at[half(k, 1)], yd
        elif kind == 2:
            src, dst, p = xa.at[yu, gs], r2d.at[gs], yu
        else:
            src, dst, p = xa.at[yd, gs], r2u.at[gs], yd
        return ycopy(src, dst, rs_s.at[kind, k], rs_r.at[kind, k], p)

    def rs_in(kind, k):
        dst = r1.at[half(k, kind)] if kind < 2 else (r2d, r2u)[kind - 2].at[pl.ds(group_in(k) * gc, gc)]
        return ycopy(dst, dst, rs_s.at[kind, k], rs_r.at[kind, k], y)

    rbuf = (retA, retB)

    def result(kind, n, count):
        n = pl.ds(n * cpn, count * cpn)
        return xa.at[y, n] if kind == 0 else xb.at[n, :, pl.ds(0, b)]

    def rx(kind, k, p):
        z = lax.rem(mz + near[p], nz)
        src = result(kind, group_in(k) * gn + 2 * z, 2)
        dst = rbuf[kind].at[pl.ds((stage(k) * gn + 2 * z) * cpn, 2 * cpn)]
        return ncopy(src, dst, rx_s.at[kind, k - 1, p], rx_r.at[kind, k - 1, p], group_in(k) * gn + q)

    def rz(kind, k, p, h):
        to = peer_out(p, h)
        src = result(kind, mx * gn + to, 1) if k == 0 else rbuf[kind].at[cells(stage(k) * gn + to)]
        dst = rbuf[kind].at[cells(group_out(k) * gn + q)]
        return ncopy(src, dst, rz_s.at[kind, k], rz_r.at[kind, k], mx * gn + to)

    def all_back(kind, k):
        ref = rbuf[kind].at[pl.ds(0, (gn - 1) * cpn)]
        return ncopy(ref, ref, rz_s.at[kind, k], rz_r.at[kind, k], me)

    def back(kind, k, p):
        with jax.named_scope("back%d" % kind):
            if k > 0:
                rx(kind, k, p).wait_recv()
            if p > 0:
                rz(kind, k, p, 0).start()
            rz(kind, k, p, 1).start()
            if p == 0:
                to = cells(group_out(k) * gn + q)
                if k > 0:
                    rbuf[kind][to] = rbuf[kind][cells(stage(k) * gn + q)]
                elif kind == 0:
                    retA[to] = xa[y, to]
                else:
                    retB[to] = xb[to, :, pl.ds(0, b)]

    def sum_far(k):
        h0, h1 = half(k, 0), half(k, 1)
        with jax.named_scope("sum_far"):
            rs_in(0, k).wait_recv()
            xa[yu, h0] = (xa[yu, h0].astype(F32) + r1[h0].astype(F32)).astype(BF16)
            rs(2, k).start()
            rs_in(1, k).wait_recv()
            xa[yd, h1] = (xa[yd, h1].astype(F32) + r1[h1].astype(F32)).astype(BF16)
            rs(3, k).start()

    def sum_near(k):
        gs = pl.ds(group_in(k) * gc, gc)
        with jax.named_scope("sum_near"):
            rs_in(2, k).wait_recv()
            rs_in(3, k).wait_recv()
            xa[y, gs] = (xa[y, gs].astype(F32) + r2d[gs].astype(F32) + r2u[gs].astype(F32)).astype(BF16)
        for p in (1, 2, 3, 0):
            if k == 0:
                back(0, 0, p)
            else:
                rx(0, k, p).start()

    def experts(k):
        g = group_in(k)
        gs = pl.ds(g * gc, gc)
        glane = lax.broadcasted_iota(jnp.int32, (gr, 128), 1)
        gall = xb[gs, :, pl.ds(b, 128)].astype(F32).reshape(gr, 128)
        gate = [jnp.sum(jnp.where(glane == n_node + me * n_exp + e, gall, 0.0), axis=1, keepdims=True) for e in range(n_exp)]
        planes = jnp.concatenate([xa[s, gs].reshape(gr, a) for s in range(n_loc)], axis=0)
        for s in range(n_loc):
            xs[:, pl.ds(s * a, a)] = jnp.dot(turn[s], planes, preferred_element_type=F32).astype(BF16)
        x = jnp.concatenate([xs[...], xb[gs, :, pl.ds(0, b)].reshape(gr, b)], axis=1)
        for c in range(0, hid, 256):
            w = min(256, hid - c)
            v = jnp.dot(x, upv[:, pl.ds(c, w)], preferred_element_type=F32)
            for j in range(0, w, 128):
                u = v[:, j : j + 128]
                hs[:, pl.ds(c + j, 128)] = (u / (1.0 + jnp.exp(-u)) * gate[(c + j) // ff]).astype(BF16)
        for s in range(n_loc):
            v = jnp.dot(hs[...], dnv[:, pl.ds(s * a, a)], preferred_element_type=F32)
            ps[pl.ds(s * gr, gr), :] = v.astype(BF16)
        for c in range(0, b, btile):
            v = jnp.dot(hs[...], dnv[:, pl.ds(n_loc * a + c, btile)], preferred_element_type=F32)
            xb[gs, :, pl.ds(c, btile)] = v.astype(BF16).reshape(gc, 8, btile)
        for s in range(n_loc):
            v = jnp.dot(turn[s], ps[...], preferred_element_type=F32)
            xa[s, gs] = v.astype(BF16).reshape(gc, 8, a)

    def relay(kind, *ks):
        def steps(p):
            with jax.named_scope("relay%d" % kind):
                for k in ks:
                    forward(kind, k, p)
        return steps

    for k in (1, 2):
        near_leg(0, k)
    for p in range(nz):
        forward(0, 0, p)
    for c in ws:
        c.start()
    place = lax.broadcasted_iota(jnp.int32, (gn, blk, n_loc * gr), 1).astype(F32)
    node_row = lax.broadcasted_iota(jnp.int32, (gn, blk, n_loc * gr), 0).astype(F32)
    column = lax.broadcasted_iota(jnp.int32, (gn, blk, n_loc * gr), 2).astype(F32)
    first = jnp.floor((place + 0.5) * (1.0 / cap)) * (gr - cap) + place + node_row * blk
    for s in range(n_loc):
        turn[s] = jnp.where(column == first + s * cap, 1.0, 0.0).reshape(gr, n_loc * gr).astype(BF16)
    with jax.named_scope("wait_meta"):
        all_tokens(0).wait_recv()
    placing(ym[...].reshape(toks, 128), sel, selT)
    for p in range(nz):
        relay(0, 1, 2)(p)
    far_leg(0, 0, 1, 2, 3)
    spread(0)
    with jax.named_scope("wait_yB"):
        all_tokens(1).wait_recv()
    for k in (1, 2):
        select(k)
        near_leg(1, k)
    select(0)
    for p in range(nz):
        forward(1, 0, p)
    select(3)
    for p in range(nz):
        relay(0, 3)(p)
    spread(1)
    spread_far(0)
    relay(1, 1, 2)(0)
    spread(2)
    relay(1, 1, 2)(1)
    spread_far(1)
    relay(1, 1, 2)(2)
    spread(3)
    relay(1, 1, 2)(3)
    far_leg(1, 0, 1, 2, 3)
    for c in ws:
        c.wait()

    def ready(k):
        with jax.named_scope("ready_b"):
            arrived(1, k)
        with jax.named_scope("ready_a"):
            ag_in(2, k).wait_recv()
            ag_in(3, k).wait_recv()
            for kind in range(4):
                ag(kind, k).wait_send()

    def after(k):
        if k > 0:
            rs(0, k).start()
            rs(1, k).start()
        for p in (1, 2, 3, 0):
            if k == 0:
                back(1, 0, p)
            else:
                rx(1, k, p).start()

    @pl.loop(0, ng)
    def _(i):
        for k in range(ng):
            @pl.when(i == k)
            def _():
                ready(k)

        with jax.named_scope("experts"):
            experts(i)

        @pl.when(i == 0)
        def _():
            spread_far(2)
            after(0)
            relay(1, 3)(0)

        @pl.when(i == 1)
        def _():
            after(1)
            spread_far(3)
            rs(0, 0).start()
            rs(1, 0).start()
            relay(1, 3)(1)
            relay(1, 3)(2)
            relay(1, 3)(3)

        @pl.when(i == 2)
        def _():
            after(2)
            sum_far(1)
            back(1, 1, 0)
            back(1, 1, 1)
            back(1, 1, 2)

        @pl.when(i == 3)
        def _():
            after(3)

    sum_far(2)
    back(1, 1, 3)
    back(1, 2, 0)
    back(1, 2, 1)
    back(1, 2, 2)
    back(1, 2, 3)
    sum_far(3)
    back(1, 3, 0)
    back(1, 3, 1)
    sum_near(1)
    back(1, 3, 2)
    sum_near(2)
    sum_far(0)
    back(1, 3, 3)
    for p in range(nz):
        back(0, 1, p)
    sum_near(3)

    def fin_all():
        return ycopy(fB.at[pl.ds(0, n_loc - 1)], oB.at[pl.ds(0, n_loc - 1)], f_s.at[0], f_r.at[0], y)

    def returned(kind):
        with jax.named_scope("returned%d" % kind):
            for k in range(ng):
                all_back(kind, k).wait_recv()

    returned(1)
    for c in range(0, b, btile):
        cs = pl.ds(c, btile)
        v = jnp.dot(selT[...], retB[pl.ds(0, slots // 8), :, cs].reshape(slots, btile), preferred_element_type=F32)
        fB[:, :, :, cs] = v.astype(BF16).reshape(n_loc, tr, 8, btile)
    for d in (2, 1, 3):
        p = lax.rem(y + d, n_loc)
        ycopy(fB.at[p], oB.at[y], f_s.at[0], f_r.at[0], p).start()
    oB[y] = fB[y]
    for p in range(nz):
        back(0, 2, p)
    for p in range(nz - 1):
        back(0, 3, p)
    sum_near(0)
    back(0, 3, nz - 1)
    with jax.named_scope("wait_finB"):
        fin_all().wait_recv()
    tot = oB[0].astype(F32)
    for s in range(1, n_loc):
        tot = tot + oB[s].astype(F32)
    out[:, :, pl.ds(n_loc * a, b)] = tot.astype(BF16)
    returned(0)
    v = jnp.dot(selAT[...], retA[pl.ds(0, slots // 8)].reshape(slots, a), preferred_element_type=F32)
    v = v.astype(BF16).reshape(n_loc, tr, 8, a)
    for s in range(n_loc):
        out[:, :, pl.ds(s * a, a)] = v[s]

    with jax.named_scope("drain"):
        fin_all().wait_send()
        for kind in range(2):
            all_tokens(kind).wait_send()
            for k in range(ng):
                all_forwarded(kind, k).wait_send()
                all_back(kind, k).wait_send()
                for p in range(nz):
                    if k > 0:
                        xleg(kind, k, p).wait_send()
                        rx(kind, k, p).wait_send()
        for k in range(ng):
            for kind in range(4):
                rs(kind, k).wait_send()


def body(tokens, node_ids, expert_ids, gate_weights, up_weight, down_weight):
    rows, d_model = tokens.shape
    n_node, n_loc = lax.axis_size("node"), lax.axis_size("local")
    n_exp, _, ff = up_weight.shape
    cap = node_ids.shape[1] * rows // n_node
    tr = rows // 8
    a = SLICE
    b = d_model - n_loc * a
    nb = n_node * n_loc * cap // 8
    cfg = (n_node, n_loc, cap, n_exp, tr, ff, a, b)
    slots = nb * 8
    toks = n_loc * rows
    v = lambda *s: pltpu.VMEM(s, BF16)
    dma = lambda *s: pltpu.SemaphoreType.DMA(s)
    two_legs = nb // 4 * 7
    scratch = [
        v(n_loc, tr, 8, a),
        v(n_loc, tr, 8, b),
        v(n_loc, tr, 8, 128),
        v(slots, toks),
        v(toks, slots),
        v(slots, toks),
        v(toks, slots),
        v(n_loc, slots // 4, slots),
        v(slots // 4, n_loc * a),
        v(slots, a),
        v(two_legs, 8, a),
        v(two_legs, 8, b + 128),
        v(n_loc, nb, 8, a),
        v(nb, 8, b + 128),
        v(d_model, n_exp * ff),
        v(n_exp * ff, d_model),
        v(slots // 4, n_exp * ff),
        v(nb, 8, a),
        v(nb, 8, a),
        v(nb, 8, a),
        v(two_legs, 8, a),
        v(two_legs, 8, b),
        v(n_loc, tr, 8, b),
        v(n_loc, tr, 8, b),
        dma(n_loc + 1),
        dma(2 * n_exp),
        dma(2), dma(2),
        dma(2, 3, 4), dma(2, 3, 4),
        dma(2, 4), dma(2, 4),
        dma(4, 4), dma(4, 4),
        dma(4, 4), dma(4, 4),
        dma(2, 4), dma(2, 4),
        dma(2, 3, 4), dma(2, 3, 4),
        dma(1), dma(1),
    ]
    vm = pl.BlockSpec(memory_space=pltpu.VMEM)
    hbm = pl.BlockSpec(memory_space=pl.ANY)
    out = pl.pallas_call(
        functools.partial(kernel, cfg),
        out_shape=jax.ShapeDtypeStruct((tr, 8, d_model), BF16),
        in_specs=[hbm, vm, vm, vm, hbm, hbm],
        out_specs=vm,
        scratch_shapes=scratch,
        compiler_params=pltpu.CompilerParams(collective_id=0, has_side_effects=True, vmem_limit_bytes=67043328),
    )(tokens.reshape(tr, 8, d_model), node_ids.T, expert_ids.T, gate_weights.T, up_weight, down_weight)
    return out.reshape(rows, d_model)


def solution(mesh):
    in_specs = (
        P(("node", "local"), None),
        P(("node", "local"), None),
        P(("node", "local"), None),
        P(("node", "local"), None),
        P("node", None, "local"),
        P("node", "local", None),
    )
    out_specs = P(("node", "local"), None)
    return jax.shard_map(body, mesh=mesh, in_specs=in_specs, out_specs=out_specs, check_vma=False)
```
